128 devices in a mesh: gx: 8 (over x, core), gy: 16 (over y, z).
Axes of the slice: x: 4, y: 4, z: 4, core: 2. Of those that a mesh axis runs over, the one named last changes fastest.
Arguments:
- fine_start: float32 [3, 2048, 8192], P(None, 'gx', 'gy'), may hold values from -6 to 6
- fine_known: float32 [3, 2048, 8192], P(None, 'gx', 'gy'), may hold values from -18 to 18
- fine_mu: float32 [2048, 8192], P('gx', 'gy'), may hold values from 1 to 10
- coarse_start: float32 [3, 1024, 4096], P(None, ('gx', 'gy')), may hold values from -6 to 6
- coarse_known: float32 [3, 1024, 4096], P(None, ('gx', 'gy')), may hold values from -18 to 18
- coarse_mu: float32 [1024, 4096], P(('gx', 'gy')), may hold values from 1 to 10
Outputs:
- fine_ghost: float32 [3, 2048, 8192], P(None, 'gx', 'gy')
- coarse_ghost: float32 [3, 1024, 4096], P(None, ('gx', 'gy'))
- norms: float32 [3], replicated
The draws below stay inside these ranges and needn't reach their ends.
All inputs are finite; a program needn't handle non-finite values.
Results may differ from the reference program's by a relative error of at most 0.0001.
Values sent between devices are 32-bit elements; how exact they have to be, the bound alone decides.
No kernel may reach another device: no remote copies, remote signals or barrier semaphores. Data moves between devices by JAX's collectives and lax.ppermute only.
A program may use at most 128 MiB of HBM per device.

```python
import math
import jax
import jax.numpy as jnp

ITERS = 3
NCX = 1024
NCY = 4096
NFX = 2048
NFY = 8192


def rising_field(key, rows, cols):
    ramp = 1.0 + 2.0 * jnp.arange(rows, dtype=jnp.float32)[:, None] / max(rows - 1, 1)
    base = jnp.clip(jax.random.normal(key, (3, rows, cols), jnp.float32), -6.0, 6.0)
    return base * ramp[None]


def draw_fine_known(key, part):
    return rising_field(jax.random.fold_in(key, 11), NFX, NFY)


def draw_coarse_known(key, part):
    return rising_field(jax.random.fold_in(key, 23), NCX, NCY)


def steps_of(stream_key, extent, split, least, top_value):
    def one(dim, blocks):
        steps = jax.random.uniform(jax.random.fold_in(jax.random.fold_in(stream_key, 6), dim), (blocks,), jnp.float32, least / len(split), top_value / len(split))
        return jnp.repeat(jnp.exp(steps), extent[dim] // blocks).reshape((-1,) + (1,) * (len(extent) - dim - 1))

    gain = one(*split[0])
    for cut in split[1:]:
        gain = gain * one(*cut)
    return gain


def bell_draw(key, extent, spread, limit, split=(), kind=jnp.bfloat16):
    factor_of = steps_of(key, extent, split, -0.22, 0.18) if split else 1.0
    drawn = jax.random.normal(key, extent, jnp.float32) * spread * factor_of
    return jnp.minimum(jnp.maximum(drawn, -limit), limit).astype(kind)


def setup_inputs(seed: int = 0) -> dict:
    arg_keys = jax.random.split(jax.random.key(seed), 7)
    return {
        "fine_start": bell_draw(arg_keys[0], (3, NFX, NFY), 1.0, 6.0, ((1, 8), (2, 16)), jnp.float32),
        "fine_known": draw_fine_known(jax.random.fold_in(arg_keys[6], 71), 0),
        "fine_mu": jnp.clip(jnp.exp(math.log(10.0) - 2.3025851 * jax.random.uniform(arg_keys[2], (NFX, NFY), jnp.float32) ** steps_of(arg_keys[2], (NFX, NFY), ((0, 8), (1, 16)), -0.2, 0.2)), 1.0, 10.0),
        "coarse_start": bell_draw(arg_keys[3], (3, NCX, NCY), 1.0, 6.0, ((1, 128),), jnp.float32),
        "coarse_known": draw_coarse_known(jax.random.fold_in(arg_keys[6], 71), 0),
        "coarse_mu": jnp.clip(jnp.exp(math.log(10.0) - 2.3025851 * jax.random.uniform(arg_keys[5], (NCX, NCY), jnp.float32) ** steps_of(arg_keys[5], (NCX, NCY), ((0, 128),), -0.2, 0.2)), 1.0, 10.0),
    }


def neighbours(padded):
    return padded[:, 2:, 1:-1] + padded[:, :-2, 1:-1] + padded[:, 1:-1, 2:] + padded[:, 1:-1, :-2]

def prolong(padded):
    components, rows_plus, cols_plus = padded.shape
    middle = padded[:, 1:-1, :]
    even_rows = 0.75 * middle + 0.25 * padded[:, :-2, :]
    odd_rows = 0.75 * middle + 0.25 * padded[:, 2:, :]
    row_fine = jnp.stack([even_rows, odd_rows], axis=2).reshape(components, 2 * (rows_plus - 2), cols_plus)
    centre = row_fine[:, :, 1:-1]
    even_cols = 0.75 * centre + 0.25 * row_fine[:, :, :-2]
    odd_cols = 0.75 * centre + 0.25 * row_fine[:, :, 2:]
    return jnp.stack([even_cols, odd_cols], axis=3).reshape(components, 2 * (rows_plus - 2), 2 * (cols_plus - 2))

def restrict(fine):
    return 0.25 * (fine[:, 0::2, 0::2] + fine[:, 1::2, 0::2] + fine[:, 0::2, 1::2] + fine[:, 1::2, 1::2])

def pad_plane(field):
    return jnp.pad(field, ((0, 0), (1, 1), (1, 1)))

def reference(fine_start, fine_known, fine_mu, coarse_start, coarse_known, coarse_mu):
    fine_diag = (fine_mu + 1.0)[None]
    coarse_diag = (coarse_mu + 1.0)[None]
    fine_ghost = fine_start
    coarse_ghost = coarse_start
    cell_total = 3.0 * (NFX * NFY + NCX * NCY)
    norm_list = []
    for sweep in range(ITERS):
        coarse_padded = pad_plane(coarse_ghost)
        fine_res = fine_known + 0.25 * neighbours(pad_plane(fine_ghost)) + 0.5 * prolong(coarse_padded) - fine_diag * fine_ghost
        coarse_res = coarse_known + 0.25 * neighbours(coarse_padded) + 0.5 * restrict(fine_ghost) - coarse_diag * coarse_ghost
        total = jnp.sum(fine_res * fine_res) + jnp.sum(coarse_res * coarse_res)
        norm_list.append(jnp.sqrt(total / cell_total))
        fine_ghost = fine_ghost + fine_res / fine_diag
        coarse_ghost = coarse_ghost + coarse_res / coarse_diag
    return (fine_ghost, coarse_ghost, jnp.stack(norm_list))
```

```python
import jax
import jax.numpy as jnp
from jax import lax
from jax.experimental import pallas as pl
from jax.experimental.pallas import tpu as pltpu
from jax.sharding import PartitionSpec as P

ITERS = 3
GX, GY = "gx", "gy"
BOTH = (GX, GY)
PR = 128
TOP = 16
ROWS = PR + 2 * TOP
F32 = jnp.float32
BF16 = jnp.bfloat16
VMEM = pl.BlockSpec(memory_space=pltpu.VMEM)
SMEM = pl.BlockSpec(memory_space=pltpu.SMEM)
ANY = pl.BlockSpec(memory_space=pl.ANY)
LIMIT = 56 * 1024 * 1024


def shaped(*shape):
    return jax.ShapeDtypeStruct(shape, F32)


def params(**kw):
    return pltpu.CompilerParams(vmem_limit_bytes=LIMIT, **kw)


def cost(us, moved):
    return pl.CostEstimate(flops=int(us * 7.0e6), bytes_accessed=int(moved), transcendentals=0)


def lanes_of(rows):
    return lax.broadcasted_iota(jnp.int32, (rows, 128), 1)


def turn(x, shift):
    shift %= 128
    return x if shift == 0 else pltpu.roll(x, shift, axis=1)


MAIN = 120
TAIL = 40
HALO_ROWS = 17


def planes_of(start_ref, known_ref, mu_ref):
    def tile(p, t):
        cols = pl.ds(128 * t, 128)
        if p < 3:
            return start_ref[p, :, cols]
        if p < 6:
            return known_ref[p - 3, :, cols]
        return mu_ref[:, cols]

    return tile


def pack_kernel(first_ref, start_ref, known_ref, mu_ref, chunk_ref, edge_ref):
    tile = planes_of(start_ref, known_ref, mu_ref)
    lane = lanes_of(8)
    zero = jnp.zeros((8, 128), F32)
    first = first_ref[0] == 1

    def ends(x):
        return jnp.where(first, x[0:3], x[5:8])

    for j in range(16):
        side = zero
        for p in range(7):
            left = tile(p, 2 * j - 1) if j else zero
            right = tile(p, 2 * j + 2) if j < 15 else zero
            both = jnp.where(lane >= 125, left, right)
            side = jnp.where((lane >= 6 * p) & (lane < 6 * p + 6), turn(both, 6 * p + 3), side)
            for m in range(2):
                x = tile(p, 2 * j + m)
                chunk_ref[j, pl.ds((2 * p + m) * 8, 8), :] = x
                if p < 3:
                    edge_ref[j, pl.ds(m * HALO_ROWS + 3 * p, 3), :] = ends(x)
                else:
                    two = jnp.where(first, x[0:2], x[6:8])
                    edge_ref[j, pl.ds(m * HALO_ROWS + 3 + 2 * p, 2), :] = two
        chunk_ref[j, pl.ds(112, 8), :] = side
        edge_ref[j, pl.ds(2 * HALO_ROWS, 3), :] = ends(side)
        edge_ref[j, pl.ds(2 * HALO_ROWS + 3, 3), :] = jnp.zeros((3, 128), F32)


def tail_kernel(edge_ref, chunk_in, chunk_ref, sem):
    del chunk_in
    copy = pltpu.make_async_copy(edge_ref, chunk_ref.at[:, pl.ds(MAIN, TAIL), :], sem)
    copy.start()
    copy.wait()


def split3(x):
    a = x.astype(BF16)
    r = x - a.astype(F32)
    b = r.astype(BF16)
    return a, b, (r - b.astype(F32)).astype(BF16)


def permuted(x, table):
    a, b, c = split3(x)
    dot = lambda v: jnp.dot(v, table, preferred_element_type=F32)
    return dot(a) + dot(b) + dot(c)


def parity_table(forward):
    one = lax.broadcasted_iota(jnp.int32, (256, 256), 0 if forward else 1)
    two = lax.broadcasted_iota(jnp.int32, (256, 256), 1 if forward else 0)
    place = jnp.where(two < 128, 2 * two, 2 * two - 255)
    return jnp.where(one == place, 1.0, 0.0).astype(BF16)


def fine_kernel(
    start_hbm, known_hbm, mu_hbm, fs_ref, fk_ref, fm_ref, low_ref, high_ref, top_ref, bottom_ref, block, sems
):
    copies = []
    for k in range(7):
        source = (start_hbm.at[k] if k < 3 else None, known_hbm.at[k - 3] if 3 <= k < 6 else None, mu_hbm)[
            0 if k < 3 else 1 if k < 6 else 2
        ]
        for c in range(4):
            n = 4 * k + c
            copies.append(pltpu.make_async_copy(source.at[:, pl.ds(128 * c, 128)], block.at[k, c], sems.at[n]))
    for copy in copies:
        copy.start()
    table = parity_table(True)
    lane = lanes_of(PR)
    low_ref[...] = jnp.zeros((PR, 128), F32)
    high_ref[...] = jnp.zeros((PR, 128), F32)

    def put(ref, mask, value):
        ref[...] = jnp.where(mask, value, ref[...])

    for k in range(7):
        for copy in copies[4 * k : 4 * k + 4]:
            copy.wait()
        out, t0 = (fs_ref, fk_ref, fm_ref)[k // 3], 4 * k - 12 * (k // 3)
        for p in range(2):
            rows = pl.ds(p, PR, stride=2)
            for m in range(2):
                x = jnp.concatenate([block[k, 2 * m + c, rows, :] for c in range(2)], axis=1)
                y = permuted(x, table)
                for q in range(2):
                    t = t0 + 2 * p + q
                    v = y[:, 128 * q : 128 * q + 128]
                    out[t, m, :, :] = v
                    if k < 3:
                        top_ref[m, pl.ds(2 * t, 2), :] = v[0:2]
                        bottom_ref[m, pl.ds(2 * t, 2), :] = v[126:128]
                        if m == 0:
                            put(low_ref, (lane == 4 * t + 2) | (lane == 4 * t + 3), turn(v, 4 * t + 2))
                        else:
                            put(high_ref, (lane == 4 * t) | (lane == 4 * t + 1), turn(v, 4 * t - 126))
                    else:
                        row, at = (24 + t, 48 + 2 * t) if k < 6 else (36 + t, 72 + 2 * t)
                        top_ref[m, pl.ds(row, 1), :] = v[0:1]
                        bottom_ref[m, pl.ds(row, 1), :] = v[127:128]
                        if m == 0:
                            put(low_ref, lane == at + 1, turn(v, at + 1))
                        else:
                            put(high_ref, lane == at, turn(v, at - 127))


def start_side(x, t):
    lane = lanes_of(x.shape[0])
    return jnp.where((lane < 2) | (lane >= 126), turn(x, 126 - 4 * t), 0.0)


def other_side(x, at):
    lane = lanes_of(x.shape[0])
    return jnp.where((lane < 1) | (lane >= 127), turn(x, 127 - at), 0.0)


def rows_kernel(left_ref, right_ref, top_ref, bottom_ref, up_ref, down_ref):
    for part, out, two, one in ((top_ref, up_ref, 0, 0), (bottom_ref, down_ref, 126, 127)):
        out[0:2] = part[...]
        pair = left_ref[two : two + 2] + right_ref[two : two + 2]
        single = left_ref[one : one + 1] + right_ref[one : one + 1]
        for t in range(12):
            out[2, pl.ds(2 * t, 2), :] = start_side(pair, t)
            out[2, pl.ds(24 + t, 1), :] = other_side(single, 48 + 2 * t)
        for t in range(4):
            out[2, pl.ds(36 + t, 1), :] = other_side(single, 72 + 2 * t)


def sweep_kernel(
    fs_hbm, fk_hbm, fm_hbm, recv_ref, left_ref, right_ref, above_ref, below_ref,
    chunk_ref, fine_ref,
    ca, cb, kc, mc, rc, fa, fb, kf, mf, rf, sems,
):
    own = pl.ds(TOP, PR)
    copies = [
        pltpu.make_async_copy(src, dst.at[:, pl.ds(0, 2), own, :], sems.at[n])
        for n, (src, dst) in enumerate(((fs_hbm, fa), (fk_hbm, kf), (fm_hbm, mf)))
    ]
    for copy in copies:
        copy.start()
    zero8 = jnp.zeros((8, 128), F32)
    for ref, count in ((ca, 3), (cb, 3), (kc, 3), (fa, 12), (fb, 12), (kf, 12), (mf, 4)):
        for t in range(count):
            for m in range(3):
                for r in (0, 8, TOP + PR, TOP + PR + 8):
                    ref[t, m, pl.ds(r, 8), :] = zero8
    for m in range(3):
        for r in (0, 8, TOP + PR, TOP + PR + 8):
            mc[m, pl.ds(r, 8), :] = zero8
    lane8 = lanes_of(8)
    wide = (lane8 < 3) | (lane8 >= 125)

    def coarse(p):
        return (ca.at[p], kc.at[p - 3] if 3 <= p < 6 else None, mc)[0 if p < 3 else 1 if p < 6 else 2]

    for p in range(7):
        ref = coarse(p)
        for j in range(16):
            rows = pl.ds(TOP + 8 * j, 8)
            for m in range(2):
                ref[m, rows, :] = recv_ref[j, pl.ds((2 * p + m) * 8, 8), :]
            ref[2, rows, :] = jnp.where(wide, turn(recv_ref[j, pl.ds(112, 8), :], 125 - 6 * p), 0.0)
        count = 3 if p < 3 else 2
        h = 3 * p if p < 3 else 3 + 2 * p
        side = MAIN + 2 * HALO_ROWS
        for j, at, skip in ((0, TOP - count, 3 - count), (15, TOP + PR, 0)):
            rows = pl.ds(at, count)
            for m in range(2):
                ref[m, rows, :] = recv_ref[j, pl.ds(MAIN + m * HALO_ROWS + h, count), :]
            lane = lanes_of(count)
            halo = turn(recv_ref[j, pl.ds(side + skip, count), :], 125 - 6 * p)
            ref[2, rows, :] = jnp.where((lane < 3) | (lane >= 125), halo, 0.0)
    both = left_ref[...] + right_ref[...]
    for t in range(12):
        fa[t, 2, own, :] = start_side(both, t)
        kf[t, 2, own, :] = other_side(both, 48 + 2 * t)
    for t in range(4):
        mf[t, 2, own, :] = other_side(both, 72 + 2 * t)
    for m in range(3):
        for t in range(12):
            fa[t, m, pl.ds(TOP - 2, 2), :] = above_ref[m, pl.ds(2 * t, 2), :]
            fa[t, m, pl.ds(TOP + PR, 2), :] = below_ref[m, pl.ds(2 * t, 2), :]
            kf[t, m, pl.ds(TOP - 1, 1), :] = above_ref[m, pl.ds(24 + t, 1), :]
            kf[t, m, pl.ds(TOP + PR, 1), :] = below_ref[m, pl.ds(24 + t, 1), :]
        for t in range(4):
            mf[t, m, pl.ds(TOP - 1, 1), :] = above_ref[m, pl.ds(36 + t, 1), :]
            mf[t, m, pl.ds(TOP + PR, 1), :] = below_ref[m, pl.ds(36 + t, 1), :]
    for copy in copies:
        copy.wait()

    def inverse(i, _):
        r = pl.ds(pl.multiple_of(8 + 8 * i, 8), 8)
        for m in range(3):
            mu = mc[m, r, :]
            rc[m, r, :] = jnp.where(mu > 0.0, 1.0 / (mu + 1.0), 0.0)
            for t in range(4):
                mu = mf[t, m, r, :]
                rf[t, m, r, :] = jnp.where(mu > 0.0, 1.0 / (mu + 1.0), 0.0)
        return 0

    lax.fori_loop(0, ROWS // 8 - 2, inverse, 0)
    at_start, at_end = lane8 == 0, lane8 == 127

    def before(x, tiles):
        turned = [turn(v, 1) for v in x]
        return [jnp.where(at_start, turned[m - 1], turned[m]) for m in tiles]

    def after(x, tiles):
        turned = [turn(v, 127) for v in x]
        return [jnp.where(at_end, turned[(m + 1) % 3], turned[m]) for m in tiles]

    def step(r, c_old, f_old, store_c, store_f, tiles, sums):
        here, up, down = pl.ds(r, 8), pl.ds(r - 1, 8), pl.ds(r + 1, 8)
        every = range(3)
        totals = [zero8] * 4
        for k in range(3):
            c = [c_old[k, m, here, :] for m in every]
            cu = [c_old[k, m, up, :] for m in every]
            cd = [c_old[k, m, down, :] for m in every]
            cw, ce = before(c, tiles), after(c, tiles)
            f = [[[f_old[4 * k + 2 * p + q, m, here, :] for m in every] for q in range(2)] for p in range(2)]
            for p in range(2):
                row = [0.375 * c[m] + 0.125 * (cu, cd)[p][m] for m in every]
                quarter = [0.25 * v for v in row]
                for q in range(2):
                    t = 4 * k + 2 * p + q
                    beside = (before, after)[q](quarter, tiles)
                    far = (before, after)[q](f[p][1 - q], tiles)
                    for n, m in enumerate(tiles):
                        v = f[p][q][m]
                        other = f_old[4 * k + 2 * (1 - p) + q, m, (up, down)[p], :]
                        near = (f[1 - p][q][m] + other) + (f[p][1 - q][m] + far[n])
                        s = (kf[t, m, here, :] + 0.25 * near) + (0.75 * row[m] + beside[n])
                        store_f(t, m, s * rf[2 * p + q, m, here, :])
                        if sums and m < 2:
                            res = s - (mf[2 * p + q, m, here, :] + 1.0) * v
                            totals[2 * p + q] = totals[2 * p + q] + res * res
            for n, m in enumerate(tiles):
                near = (cu[m] + cd[m]) + (cw[n] + ce[n])
                four = (f[0][0][m] + f[0][1][m]) + (f[1][0][m] + f[1][1][m])
                s = (kc[k, m, here, :] + 0.25 * near) + 0.125 * four
                store_c(k, m, s * rc[m, here, :])
                if sums and m < 2:
                    res = s - (mc[m, here, :] + 1.0) * c[m]
                    totals[k] = totals[k] + res * res
        return (totals[0] + totals[1]) + (totals[2] + totals[3])

    def sweep(c_old, f_old, c_new, f_new):
        def store(r):
            def store_c(k, m, v):
                c_new[k, m, pl.ds(r, 8), :] = v

            def store_f(t, m, v):
                f_new[t, m, pl.ds(r, 8), :] = v

            return store_c, store_f

        def body(i, total):
            r = pl.multiple_of(TOP + 8 * i, 8)
            return total + step(r, c_old, f_old, *store(r), range(3), True)

        total = lax.fori_loop(0, PR // 8, body, zero8)

        def edge(i, carry):
            r = pl.multiple_of(TOP - 8 + i * (PR + 8), 8)
            step(r, c_old, f_old, *store(r), range(3), False)
            return carry

        lax.fori_loop(0, 2, edge, 0)
        return total

    totals = [sweep(ca, fa, cb, fb), sweep(cb, fb, ca, fa)]

    def last(i, total):
        r = pl.multiple_of(TOP + 8 * i, 8)

        def store_c(k, m, v):
            chunk_ref[i, pl.ds((2 * k + m) * 8, 8), :] = v

        def store_f(t, m, v):
            fine_ref[t, m, pl.ds(pl.multiple_of(8 * i, 8), 8), :] = v

        return total + step(r, ca, fa, store_c, store_f, range(2), True)

    totals.append(lax.fori_loop(0, PR // 8, last, zero8))
    sums = jnp.concatenate([jnp.sum(v, axis=0, keepdims=True) for v in totals] + [jnp.zeros((5, 128), F32)], axis=0)
    for j in range(16):
        chunk_ref[j, pl.ds(48, 8), :] = sums


def join_kernel(fine_ref, out_hbm, block, sems):
    table = parity_table(False)
    copies = []
    for k in range(3):
        for m in range(2):
            for p in range(2):
                x = jnp.concatenate([fine_ref[4 * k + 2 * p + q, m, :, :] for q in range(2)], axis=1)
                y = permuted(x, table)
                for c in range(2):
                    block[k, 2 * m + c, pl.ds(p, PR, stride=2), :] = y[:, 128 * c : 128 * c + 128]
            for c in range(2 * m, 2 * m + 2):
                copy = pltpu.make_async_copy(
                    block.at[k, c], out_hbm.at[k, :, pl.ds(128 * c, 128)], sems.at[4 * k + c]
                )
                copy.start()
                copies.append(copy)
    for copy in copies:
        copy.wait()


def sum_kernel(recv_ref, out_ref):
    total = recv_ref[0]
    for j in range(1, 16):
        total = total + recv_ref[j]
    for i in range(8):
        out_ref[i] = total


def coarse_kernel(recv_ref, out_ref):
    for j in range(16):
        for k in range(3):
            for m in range(2):
                out_ref[k, :, pl.ds(256 * j + 128 * m, 128)] = recv_ref[j, pl.ds((2 * k + m) * 8, 8), :]


def on_device(fine_start, fine_known, fine_mu, coarse_start, coarse_known, coarse_mu):
    count_x, count_y = lax.axis_size(GX), lax.axis_size(GY)
    cell_total = 3.0 * (fine_mu.size + coarse_mu.size) * (count_x * count_y)
    first = (lax.axis_index(GY) == 0).astype(jnp.int32).reshape(1)

    chunk, edge = pl.pallas_call(
        pack_kernel,
        out_shape=(shaped(16, MAIN + TAIL, 128), shaped(16, TAIL, 128)),
        in_specs=[SMEM, VMEM, VMEM, VMEM],
        out_specs=(VMEM, VMEM),
        compiler_params=params(),
        cost_estimate=cost(2, 2.5e6),
        name="pack",
    )(first, coarse_start, coarse_known, coarse_mu)
    pairs = [(i * count_y + count_y - 1, (i + 1) * count_y) for i in range(count_x - 1)]
    edge = lax.ppermute(edge, BOTH, pairs + [(b, a) for a, b in pairs])
    chunk = pl.pallas_call(
        tail_kernel,
        out_shape=shaped(16, MAIN + TAIL, 128),
        in_specs=[VMEM, ANY],
        out_specs=ANY,
        scratch_shapes=[pltpu.SemaphoreType.DMA(())],
        input_output_aliases={1: 0},
        compiler_params=params(),
        cost_estimate=cost(1, 0.6e6),
        name="tail",
    )(edge, chunk)
    recv = lax.all_to_all(chunk, GY, 0, 0, tiled=True)

    fs, fk, fm, low, high, top, bottom = pl.pallas_call(
        fine_kernel,
        out_shape=(
            shaped(12, 2, PR, 128), shaped(12, 2, PR, 128), shaped(4, 2, PR, 128),
            shaped(PR, 128), shaped(PR, 128), shaped(2, 40, 128), shaped(2, 40, 128),
        ),
        in_specs=[ANY] * 3,
        out_specs=(VMEM,) * 7,
        scratch_shapes=[pltpu.VMEM((7, 4, 2 * PR, 128), F32), pltpu.SemaphoreType.DMA((28,))],
        compiler_params=params(),
        cost_estimate=cost(4, 7e6),
        name="fine",
    )(fine_start, fine_known, fine_mu)

    def ahead(n):
        return [(i, i + 1) for i in range(n - 1)]

    def back(n):
        return [(i + 1, i) for i in range(n - 1)]

    left = lax.ppermute(high, GY, ahead(count_y))
    right = lax.ppermute(low, GY, back(count_y))
    up, down = pl.pallas_call(
        rows_kernel,
        out_shape=(shaped(3, 40, 128),) * 2,
        in_specs=[VMEM] * 4,
        out_specs=(VMEM,) * 2,
        compiler_params=params(),
        cost_estimate=cost(1, 0.3e6),
        name="rows",
    )(left, right, top, bottom)
    above = lax.ppermute(down, GX, ahead(count_x))
    below = lax.ppermute(up, GX, back(count_x))

    chunk, fine = pl.pallas_call(
        sweep_kernel,
        out_shape=(shaped(16, 56, 128), shaped(12, 2, PR, 128)),
        in_specs=[ANY] * 3 + [VMEM] * 5,
        out_specs=(VMEM,) * 2,
        scratch_shapes=[
            pltpu.VMEM((3, 3, ROWS, 128), F32),
            pltpu.VMEM((3, 3, ROWS, 128), F32),
            pltpu.VMEM((3, 3, ROWS, 128), F32),
            pltpu.VMEM((3, ROWS, 128), F32),
            pltpu.VMEM((3, ROWS, 128), F32),
            pltpu.VMEM((12, 3, ROWS, 128), F32),
            pltpu.VMEM((12, 3, ROWS, 128), F32),
            pltpu.VMEM((12, 3, ROWS, 128), F32),
            pltpu.VMEM((4, 3, ROWS, 128), F32),
            pltpu.VMEM((4, 3, ROWS, 128), F32),
            pltpu.SemaphoreType.DMA((3,)),
        ],
        compiler_params=params(),
        cost_estimate=cost(8, 7e6),
        name="sweeps",
    )(fs, fk, fm, recv, left, right, above, below)
    out = lax.all_to_all(chunk, GY, 0, 0, tiled=True)

    fine_ghost = pl.pallas_call(
        join_kernel,
        out_shape=shaped(*fine_start.shape),
        in_specs=[VMEM],
        out_specs=ANY,
        scratch_shapes=[pltpu.VMEM((3, 4, 2 * PR, 128), F32), pltpu.SemaphoreType.DMA((12,))],
        compiler_params=params(),
        cost_estimate=cost(2, 3e6),
        name="join",
    )(fine)
    sums = pl.pallas_call(
        sum_kernel,
        grid=(1,),
        out_shape=shaped(8, 8, 128),
        in_specs=[pl.BlockSpec((16, 8, 128), lambda i: (0, 6, 0))],
        out_specs=pl.BlockSpec((8, 8, 128), lambda i: (0, 0, 0)),
        compiler_params=params(),
        cost_estimate=cost(1, 0.1e6),
        name="sums",
    )(out)
    sums = lax.all_to_all(sums, GX, 0, 0, tiled=True)
    coarse_ghost = pl.pallas_call(
        coarse_kernel,
        out_shape=shaped(*coarse_start.shape),
        in_specs=[VMEM],
        out_specs=VMEM,
        compiler_params=params(),
        cost_estimate=cost(1, 0.8e6),
        name="coarse",
    )(out)
    norms = jnp.sqrt(jnp.sum(sums[:, :ITERS, :], axis=(0, 2)) / cell_total)
    return fine_ghost, coarse_ghost, norms


def solution(mesh):
    fine, coarse = P(None, GX, GY), P(None, BOTH, None)
    return jax.shard_map(
        on_device,
        mesh=mesh,
        in_specs=(fine, fine, P(GX, GY), coarse, coarse, P(BOTH, None)),
        out_specs=(fine, coarse, P()),
        check_vma=False,
    )
```

```python
import jax
import jax.numpy as jnp
from jax import lax
from jax.experimental import pallas as pl
from jax.experimental.pallas import tpu as pltpu
from jax.sharding import PartitionSpec as P

ITERS = 3
GX, GY = "gx", "gy"
BOTH = (GX, GY)
PR = 128
TOP = 16
ROWS = PR + 2 * TOP
F32 = jnp.float32
BF16 = jnp.bfloat16
VMEM = pl.BlockSpec(memory_space=pltpu.VMEM)
HBM = pl.BlockSpec(memory_space=pltpu.HBM)


def shaped(*shape):
    return jax.ShapeDtypeStruct(shape, F32)


ALL_KIB = 65472


def params(kib):
    return pltpu.CompilerParams(vmem_limit_bytes=kib << 10)


def cost(us, moved):
    return pl.CostEstimate(flops=int(us * 7.0e6), bytes_accessed=int(moved), transcendentals=0)


def in_hbm(*arrays):
    return tuple(pltpu.with_memory_space_constraint(a, pltpu.HBM) for a in arrays)


def lanes_of(rows):
    return lax.broadcasted_iota(jnp.int32, (rows, 128), 1)


def turn(x, shift):
    shift %= 128
    return x if shift == 0 else pltpu.roll(x, shift, axis=1)


MAIN = 120
EDGE = 64


def edge_rows(p):
    return (40 + 3 * p, 3) if p < 3 else (43 + 2 * p, 2)


def planes_of(start_ref, known_ref, mu_ref):
    def tile(p, t):
        cols = pl.ds(128 * t, 128)
        if p < 3:
            return start_ref[p, :, cols]
        if p < 6:
            return 4.0 * known_ref[p - 3, :, cols]
        return 4.0 * mu_ref[:, cols]

    return tile


def pack_kernel(start_hbm, known_hbm, mu_hbm, chunk_ref, start_ref, known_ref, mu_ref, sems):
    copies = [
        pltpu.make_async_copy(src, dst, sems.at[n])
        for n, (src, dst) in enumerate(((start_hbm, start_ref), (known_hbm, known_ref), (mu_hbm, mu_ref)))
    ]
    for copy in copies:
        copy.start()
    for copy in copies:
        copy.wait()
    tile = planes_of(start_ref, known_ref, mu_ref)
    lane = lanes_of(8)
    zero = jnp.zeros((8, 128), F32)
    for j in range(16):
        side = zero
        for p in range(7):
            left = tile(p, 2 * j - 1) if j else zero
            right = tile(p, 2 * j + 2) if j < 15 else zero
            both = jnp.where(lane >= 125, left, right)
            side = jnp.where((lane >= 6 * p) & (lane < 6 * p + 6), turn(both, 6 * p + 3), side)
            for m in range(2):
                chunk_ref[j, pl.ds((2 * p + m) * 8, 8), :] = tile(p, 2 * j + m)
        chunk_ref[j, pl.ds(112, 8), :] = side


def beside(x, p):
    lane = lanes_of(x.shape[0])
    return jnp.where((lane < 3) | (lane >= 125), turn(x, 125 - 6 * p), 0.0)


def split3(x):
    a = x.astype(BF16)
    r = x - a.astype(F32)
    b = r.astype(BF16)
    return a, b, (r - b.astype(F32)).astype(BF16)


def permuted(x, table):
    a, b, c = split3(x)
    dot = lambda v: jnp.dot(v, table, preferred_element_type=F32)
    return dot(a) + dot(b) + dot(c)


def parity_table(forward, value=1.0):
    one = lax.broadcasted_iota(jnp.int32, (256, 256), 0 if forward else 1)
    two = lax.broadcasted_iota(jnp.int32, (256, 256), 1 if forward else 0)
    place = jnp.where(two < 128, 2 * two, 2 * two - 255)
    return jnp.where(one == place, value, 0.0).astype(BF16)


def fine_kernel(
    start_hbm, known_hbm, mu_hbm, fs_hbm, fk_hbm, fm_hbm, low_ref, high_ref, top_ref, bottom_ref,
    block, planes, sems, out_sems,
):
    copies = []
    for k in range(7):
        source = (start_hbm.at[k] if k < 3 else None, known_hbm.at[k - 3] if 3 <= k < 6 else None, mu_hbm)[
            0 if k < 3 else 1 if k < 6 else 2
        ]
        for c in range(4):
            n = 4 * k + c
            copies.append(pltpu.make_async_copy(source.at[:, pl.ds(128 * c, 128)], block.at[k, c], sems.at[n]))
    for copy in copies:
        copy.start()
    tables = parity_table(True), parity_table(True, 4.0)
    lane = lanes_of(PR)
    low_ref[...] = jnp.zeros((PR, 128), F32)
    high_ref[...] = jnp.zeros((PR, 128), F32)

    def put(ref, mask, value):
        ref[...] = jnp.where(mask, value, ref[...])

    written = []
    for k in range(7):
        for copy in copies[4 * k : 4 * k + 4]:
            copy.wait()
        out, t0 = (fs_hbm, fk_hbm, fm_hbm)[k // 3], 4 * k - 12 * (k // 3)
        for p in range(2):
            rows = pl.ds(p, PR, stride=2)
            for m in range(2):
                x = jnp.concatenate([block[k, 2 * m + c, rows, :] for c in range(2)], axis=1)
                y = permuted(x, tables[k >= 3])
                for q in range(2):
                    t = t0 + 2 * p + q
                    v = y[:, 128 * q : 128 * q + 128]
                    planes[4 * k + 2 * p + q, m, :, :] = v
                    if k < 3:
                        top_ref[m, pl.ds(2 * t, 2), :] = v[0:2]
                        bottom_ref[m, pl.ds(2 * t, 2), :] = v[126:128]
                        if m == 0:
                            put(low_ref, (lane == 4 * t + 2) | (lane == 4 * t + 3), turn(v, 4 * t + 2))
                        else:
                            put(high_ref, (lane == 4 * t) | (lane == 4 * t + 1), turn(v, 4 * t - 126))
                    else:
                        row, at = (24 + t, 48 + 2 * t) if k < 6 else (36 + t, 72 + 2 * t)
                        top_ref[m, pl.ds(row, 1), :] = v[0:1]
                        bottom_ref[m, pl.ds(row, 1), :] = v[127:128]
                        if m == 0:
                            put(low_ref, lane == at + 1, turn(v, at + 1))
                        else:
                            put(high_ref, lane == at, turn(v, at - 127))
        written.append(pltpu.make_async_copy(planes.at[pl.ds(4 * k, 4)], out.at[pl.ds(t0, 4)], out_sems.at[k]))
        written[-1].start()
    for copy in written:
        copy.wait()


def start_side(x, t):
    lane = lanes_of(x.shape[0])
    return jnp.where((lane < 2) | (lane >= 126), turn(x, 126 - 4 * t), 0.0)


def other_side(x, at):
    lane = lanes_of(x.shape[0])
    return jnp.where((lane < 1) | (lane >= 127), turn(x, 127 - at), 0.0)


def rows_kernel(left_ref, right_ref, top_ref, bottom_ref, first_ref, last_ref, up_ref, down_ref):
    for part, patch, out, two, one in ((top_ref, first_ref, up_ref, 0, 0), (bottom_ref, last_ref, down_ref, 126, 127)):
        out[0:2, 0:40, :] = part[...]
        pair = left_ref[two : two + 2] + right_ref[two : two + 2]
        single = left_ref[one : one + 1] + right_ref[one : one + 1]
        for t in range(12):
            out[2, pl.ds(2 * t, 2), :] = start_side(pair, t)
            out[2, pl.ds(24 + t, 1), :] = other_side(single, 48 + 2 * t)
        for t in range(4):
            out[2, pl.ds(36 + t, 1), :] = other_side(single, 72 + 2 * t)
        for p in range(7):
            row, count = edge_rows(p)
            at = 0 if one == 0 else 8 - count
            for m in range(2):
                out[m, pl.ds(row, count), :] = patch[0, pl.ds((2 * p + m) * 8 + at, count), :]
            out[2, pl.ds(row, count), :] = beside(patch[0, pl.ds(112 + at, count), :], p)


def sweep_kernel(
    fs_hbm, fk_hbm, fm_hbm, recv_ref, left_ref, right_ref, above_ref, below_ref,
    chunk_ref, fine_hbm,
    ca, cb, xa, xb, kc, mc, rc, fa, fb, kf, mf, rf, fine_ref, sems, out_sems,
):
    own = pl.ds(TOP, PR)
    copies = [
        pltpu.make_async_copy(src, dst.at[:, pl.ds(0, 2), own, :], sems.at[n])
        for n, (src, dst) in enumerate(((fs_hbm, fa), (fk_hbm, kf), (fm_hbm, mf)))
    ]
    for copy in copies:
        copy.start()
    zero8 = jnp.zeros((8, 128), F32)
    for ref, count in ((ca, 3), (kc, 3), (fa, 12), (kf, 12), (mf, 4)):
        for t in range(count):
            for m in range(3):
                for r in (TOP - 8, TOP + PR):
                    ref[t, m, pl.ds(r, 8), :] = zero8
    for m in range(3):
        for r in (TOP - 8, TOP + PR):
            mc[m, pl.ds(r, 8), :] = zero8
    lane8 = lanes_of(8)

    def coarse(p):
        return (ca.at[p], kc.at[p - 3] if 3 <= p < 6 else None, mc)[0 if p < 3 else 1 if p < 6 else 2]

    for p in range(7):
        ref = coarse(p)
        for j in range(16):
            rows = pl.ds(TOP + 8 * j, 8)
            for m in range(2):
                ref[m, rows, :] = recv_ref[j, pl.ds((2 * p + m) * 8, 8), :]
            ref[2, rows, :] = beside(recv_ref[j, pl.ds(112, 8), :], p)
        row, count = edge_rows(p)
        for m in range(3):
            ref[m, pl.ds(TOP - count, count), :] = above_ref[m, pl.ds(row, count), :]
            ref[m, pl.ds(TOP + PR, count), :] = below_ref[m, pl.ds(row, count), :]
    both = left_ref[...] + right_ref[...]
    for t in range(12):
        fa[t, 2, own, :] = start_side(both, t)
        kf[t, 2, own, :] = other_side(both, 48 + 2 * t)
    for t in range(4):
        mf[t, 2, own, :] = other_side(both, 72 + 2 * t)
    for m in range(3):
        for t in range(12):
            fa[t, m, pl.ds(TOP - 2, 2), :] = above_ref[m, pl.ds(2 * t, 2), :]
            fa[t, m, pl.ds(TOP + PR, 2), :] = below_ref[m, pl.ds(2 * t, 2), :]
            kf[t, m, pl.ds(TOP - 1, 1), :] = above_ref[m, pl.ds(24 + t, 1), :]
            kf[t, m, pl.ds(TOP + PR, 1), :] = below_ref[m, pl.ds(24 + t, 1), :]
        for t in range(4):
            mf[t, m, pl.ds(TOP - 1, 1), :] = above_ref[m, pl.ds(36 + t, 1), :]
            mf[t, m, pl.ds(TOP + PR, 1), :] = below_ref[m, pl.ds(36 + t, 1), :]
    for copy in copies:
        copy.wait()

    at_start, at_end = lane8 == 0, lane8 == 127

    def before(x):
        turned = [turn(v, 1) for v in x]
        return [jnp.where(at_start, turned[m - 1], turned[m]) for m in range(len(x))]

    def after(x):
        turned = [turn(v, 127) for v in x]
        return [jnp.where(at_end, turned[(m + 1) % 3], turned[m]) for m in range(3)]

    def mix(x, k, r, c):
        west, east = before(c), after(c)
        for m in range(3):
            part = 0.375 * c[m]
            x[0, k, m, r, :] = part + 0.125 * west[m]
            x[1, k, m, r, :] = part + 0.125 * east[m]
            x[2, k, m, r, :] = west[m] + east[m]

    def ready(i, carry):
        r = pl.ds(pl.multiple_of(8 + 8 * i, 8), 8)
        for m in range(3):
            mu = mc[m, r, :]
            mc[m, r, :] = mu + 4.0
            rc[m, r, :] = jnp.where(mu > 0.0, 1.0 / (mu + 4.0), 0.0)
            for t in range(4):
                mu = mf[t, m, r, :]
                mf[t, m, r, :] = mu + 4.0
                rf[t, m, r, :] = jnp.where(mu > 0.0, 1.0 / (mu + 4.0), 0.0)
        for k in range(3):
            mix(xa, k, r, [ca[k, m, r, :] for m in range(3)])
        return carry

    lax.fori_loop(0, ROWS // 8 - 2, ready, 0)

    def step(r, c_old, x_old, f_old, store_c, store_f, tiles, sums):
        here, up, down = pl.ds(r, 8), pl.ds(r - 1, 8), pl.ds(r + 1, 8)
        totals = [zero8] * 4
        for k in range(3):
            f = [[[f_old[4 * k + 2 * p + q, m, here, :] for m in range(3)] for q in range(2)] for p in range(2)]
            far = [[(before, after)[q](f[p][1 - q]) for q in range(2)] for p in range(2)]
            new = []
            for m in range(tiles):
                for q in range(2):
                    mid = 3.0 * x_old[q, k, m, here, :]
                    for p in range(2):
                        t, side = 4 * k + 2 * p + q, (up, down)[p]
                        other = f_old[4 * k + 2 * (1 - p) + q, m, side, :]
                        near = (f[1 - p][q][m] + other) + (f[p][1 - q][m] + far[p][q][m])
                        s = (kf[t, m, here, :] + near) + (mid + x_old[q, k, m, side, :])
                        store_f(t, m, s * rf[2 * p + q, m, here, :])
                        if sums and m < 2:
                            res = s - mf[2 * p + q, m, here, :] * f[p][q][m]
                            totals[2 * p + q] = totals[2 * p + q] + res * res
                c = c_old[k, m, here, :]
                near = (c_old[k, m, up, :] + c_old[k, m, down, :]) + x_old[2, k, m, here, :]
                four = (f[0][0][m] + f[0][1][m]) + (f[1][0][m] + f[1][1][m])
                s = (kc[k, m, here, :] + 0.5 * four) + near
                new.append(s * rc[m, here, :])
                if sums and m < 2:
                    res = s - mc[m, here, :] * c
                    totals[k] = totals[k] + res * res
            store_c(k, new)
        return (totals[0] + totals[1]) + (totals[2] + totals[3])

    def sweep(c_old, x_old, f_old, c_new, x_new, f_new):
        def stores(r):
            rows = pl.ds(r, 8)

            def store_c(k, new):
                for m in range(3):
                    c_new[k, m, rows, :] = new[m]
                mix(x_new, k, rows, new)

            def store_f(t, m, v):
                f_new[t, m, rows, :] = v

            return store_c, store_f

        def body(i, total):
            r = pl.multiple_of(TOP + 8 * i, 8)
            return total + step(r, c_old, x_old, f_old, *stores(r), 3, True)

        total = lax.fori_loop(0, PR // 8, body, zero8)

        def edge(i, carry):
            r = pl.multiple_of(TOP - 8 + i * (PR + 8), 8)
            step(r, c_old, x_old, f_old, *stores(r), 3, False)
            return carry

        lax.fori_loop(0, 2, edge, 0)
        return total

    totals = [sweep(ca, xa, fa, cb, xb, fb), sweep(cb, xb, fb, ca, xa, fa)]

    def last(i, total):
        r = pl.multiple_of(TOP + 8 * i, 8)

        def store_c(k, new):
            for m in range(2):
                chunk_ref[i, pl.ds((2 * k + m) * 8, 8), :] = new[m]

        def store_f(t, m, v):
            fine_ref[t, m, pl.ds(pl.multiple_of(8 * i, 8), 8), :] = v

        return total + step(r, ca, xa, fa, store_c, store_f, 2, True)

    total, parts = zero8, 4
    written = []
    for n in range(parts):
        total = lax.fori_loop(n * PR // 8 // parts, (n + 1) * PR // 8 // parts, last, total)
        rows = pl.ds(n * PR // parts, PR // parts)
        written.append(pltpu.make_async_copy(fine_ref.at[:, :, rows], fine_hbm.at[:, :, rows], out_sems.at[n]))
        written[-1].start()
    totals.append(total)
    sums = 0.0625 * jnp.concatenate([jnp.sum(v, axis=0, keepdims=True) for v in totals] + [jnp.zeros((5, 128), F32)], axis=0)
    for j in range(16):
        chunk_ref[j, pl.ds(48, 8), :] = sums
    for copy in written:
        copy.wait()


def join_kernel(fine_hbm, out_hbm, fine_ref, block, in_sems, sems):
    reads = [
        pltpu.make_async_copy(fine_hbm.at[pl.ds(4 * k, 4)], fine_ref.at[pl.ds(4 * k, 4)], in_sems.at[k])
        for k in range(3)
    ]
    for copy in reads:
        copy.start()
    table = parity_table(False)
    copies = []
    for k in range(3):
        reads[k].wait()
        for m in range(2):
            for p in range(2):
                x = jnp.concatenate([fine_ref[4 * k + 2 * p + q, m, :, :] for q in range(2)], axis=1)
                y = permuted(x, table)
                for c in range(2):
                    block[k, 2 * m + c, pl.ds(p, PR, stride=2), :] = y[:, 128 * c : 128 * c + 128]
            for c in range(2 * m, 2 * m + 2):
                copy = pltpu.make_async_copy(
                    block.at[k, c], out_hbm.at[k, :, pl.ds(128 * c, 128)], sems.at[4 * k + c]
                )
                copy.start()
                copies.append(copy)
    for copy in copies:
        copy.wait()


def sum_kernel(recv_ref, out_ref):
    total = recv_ref[0]
    for j in range(1, 16):
        total = total + recv_ref[j]
    for i in range(8):
        out_ref[i] = total


def coarse_kernel(recv_ref, out_ref):
    for j in range(16):
        for k in range(3):
            for m in range(2):
                out_ref[k, :, pl.ds(256 * j + 128 * m, 128)] = recv_ref[j, pl.ds((2 * k + m) * 8, 8), :]


def on_device(fine_start, fine_known, fine_mu, coarse_start, coarse_known, coarse_mu):
    count_x, count_y = lax.axis_size(GX), lax.axis_size(GY)
    cell_total = 3.0 * (fine_mu.size + coarse_mu.size) * (count_x * count_y)
    chunk = pl.pallas_call(
        pack_kernel,
        out_shape=pltpu.VMEM((16, MAIN, 128), F32),
        in_specs=[HBM] * 3,
        out_specs=VMEM,
        scratch_shapes=[
            pltpu.VMEM(coarse_start.shape, F32),
            pltpu.VMEM(coarse_known.shape, F32),
            pltpu.VMEM(coarse_mu.shape, F32),
            pltpu.SemaphoreType.DMA((3,)),
        ],
        compiler_params=params(28672),
        cost_estimate=cost(2, 2e6),
        name="pack",
    )(*in_hbm(coarse_start, coarse_known, coarse_mu))
    recv = lax.all_to_all(chunk, GY, 0, 0, tiled=True)

    fs, fk, fm, low, high, top, bottom = pl.pallas_call(
        fine_kernel,
        out_shape=(
            *(pltpu.HBM((n, 2, PR, 128), F32) for n in (12, 12, 4)),
            *(pltpu.VMEM(shape, F32) for shape in ((PR, 128), (PR, 128), (2, 40, 128), (2, 40, 128))),
        ),
        in_specs=[HBM] * 3,
        out_specs=(HBM,) * 3 + (VMEM,) * 4,
        scratch_shapes=[
            pltpu.VMEM((7, 4, 2 * PR, 128), F32),
            pltpu.VMEM((28, 2, PR, 128), F32),
            pltpu.SemaphoreType.DMA((28,)),
            pltpu.SemaphoreType.DMA((7,)),
        ],
        compiler_params=params(28672),
        cost_estimate=cost(4, 7e6),
        name="fine",
    )(*in_hbm(fine_start, fine_known, fine_mu))

    def ahead(n):
        return [(i, i + 1) for i in range(n - 1)]

    def back(n):
        return [(i + 1, i) for i in range(n - 1)]

    left = lax.ppermute(high, GY, ahead(count_y))
    right = lax.ppermute(low, GY, back(count_y))
    up, down = pl.pallas_call(
        rows_kernel,
        grid=(1,),
        out_shape=(shaped(3, EDGE, 128),) * 2,
        in_specs=[pl.BlockSpec((PR, 128), lambda i: (0, 0))] * 2
        + [pl.BlockSpec((2, 40, 128), lambda i: (0, 0, 0))] * 2
        + [pl.BlockSpec((1, MAIN, 128), lambda i: (0, 0, 0)), pl.BlockSpec((1, MAIN, 128), lambda i: (15, 0, 0))],
        out_specs=(pl.BlockSpec((3, EDGE, 128), lambda i: (0, 0, 0)),) * 2,
        compiler_params=params(28672),
        cost_estimate=cost(1, 0.3e6),
        name="rows",
    )(left, right, top, bottom, recv, recv)
    above = lax.ppermute(down, GX, ahead(count_x))
    below = lax.ppermute(up, GX, back(count_x))

    chunk, fine = pl.pallas_call(
        sweep_kernel,
        out_shape=(shaped(16, 56, 128), pltpu.HBM((12, 2, PR, 128), F32)),
        in_specs=[HBM] * 3 + [VMEM] * 5,
        out_specs=(VMEM, HBM),
        scratch_shapes=[
            pltpu.VMEM((3, 3, ROWS, 128), F32),
            pltpu.VMEM((3, 3, ROWS, 128), F32),
            pltpu.VMEM((3, 3, 3, ROWS, 128), F32),
            pltpu.VMEM((3, 3, 3, ROWS, 128), F32),
            pltpu.VMEM((3, 3, ROWS, 128), F32),
            pltpu.VMEM((3, ROWS, 128), F32),
            pltpu.VMEM((3, ROWS, 128), F32),
            pltpu.VMEM((12, 3, ROWS, 128), F32),
            pltpu.VMEM((12, 3, ROWS, 128), F32),
            pltpu.VMEM((12, 3, ROWS, 128), F32),
            pltpu.VMEM((4, 3, ROWS, 128), F32),
            pltpu.VMEM((4, 3, ROWS, 128), F32),
            pltpu.VMEM((12, 2, PR, 128), F32),
            pltpu.SemaphoreType.DMA((3,)),
            pltpu.SemaphoreType.DMA((4,)),
        ],
        compiler_params=params(28672),
        cost_estimate=cost(8, 7e6),
        name="sweeps",
    )(*in_hbm(fs, fk, fm), recv, left, right, above, below)
    out = lax.all_to_all(chunk, GY, 0, 0, tiled=True)

    fine_ghost = pl.pallas_call(
        join_kernel,
        out_shape=shaped(*fine_start.shape),
        in_specs=[HBM],
        out_specs=HBM,
        scratch_shapes=[
            pltpu.VMEM((12, 2, PR, 128), F32),
            pltpu.VMEM((3, 4, 2 * PR, 128), F32),
            pltpu.SemaphoreType.DMA((3,)),
            pltpu.SemaphoreType.DMA((12,)),
        ],
        compiler_params=params(28672),
        cost_estimate=cost(2, 3e6),
        name="join",
    )(*in_hbm(fine))
    sums = pl.pallas_call(
        sum_kernel,
        grid=(1,),
        out_shape=shaped(8, 8, 128),
        in_specs=[pl.BlockSpec((16, 8, 128), lambda i: (0, 6, 0))],
        out_specs=pl.BlockSpec((8, 8, 128), lambda i: (0, 0, 0)),
        compiler_params=params(28672),
        cost_estimate=cost(1, 0.1e6),
        name="sums",
    )(out)
    sums = lax.all_to_all(sums, GX, 0, 0, tiled=True)
    coarse_ghost = pl.pallas_call(
        coarse_kernel,
        out_shape=shaped(*coarse_start.shape),
        in_specs=[VMEM],
        out_specs=VMEM,
        compiler_params=params(28672),
        cost_estimate=cost(1, 0.8e6),
        name="coarse",
    )(out)
    norms = jnp.sqrt(jnp.sum(sums[:, :ITERS, :], axis=(0, 2)) / cell_total)
    return fine_ghost, coarse_ghost, norms


def solution(mesh):
    fine, coarse = P(None, GX, GY), P(None, BOTH, None)
    return jax.shard_map(
        on_device,
        mesh=mesh,
        in_specs=(fine, fine, P(GX, GY), coarse, coarse, P(BOTH, None)),
        out_specs=(fine, coarse, P()),
        check_vma=False,
    )
```

```python
import jax
import jax.numpy as jnp
from jax import lax
from jax.experimental import pallas as pl
from jax.experimental.pallas import tpu as pltpu
from jax.sharding import PartitionSpec as P

ITERS = 3
GX, GY = "gx", "gy"
BOTH = (GX, GY)
PR = 128
TOP = 16
ROWS = PR + 40
F32 = jnp.float32
BF16 = jnp.bfloat16
VMEM = pl.BlockSpec(memory_space=pltpu.VMEM)
HBM = pl.BlockSpec(memory_space=pltpu.HBM)


def shaped(*shape):
    return jax.ShapeDtypeStruct(shape, F32)


GRANT_KIB = 36864


def params(kib):
    return pltpu.CompilerParams(vmem_limit_bytes=kib << 10)


def cost(us, moved):
    return pl.CostEstimate(flops=int(us * 7.0e6), bytes_accessed=int(moved), transcendentals=0)


def in_hbm(*arrays):
    return tuple(pltpu.with_memory_space_constraint(a, pltpu.HBM) for a in arrays)


def lanes_of(rows):
    return lax.broadcasted_iota(jnp.int32, (rows, 128), 1)


def turn(x, shift):
    shift %= 128
    return x if shift == 0 else pltpu.roll(x, shift, axis=1)


MAIN = 120
EDGE = 64


def edge_rows(p):
    return (40 + 3 * p, 3) if p < 3 else (43 + 2 * p, 2)


def planes_of(start_ref, known_ref, mu_ref):
    def tile(p, t):
        cols = pl.ds(128 * t, 128)
        if p < 3:
            return start_ref[p, :, cols]
        if p < 6:
            return 4.0 * known_ref[p - 3, :, cols]
        return 4.0 * mu_ref[:, cols]

    return tile


def pack_kernel(start_hbm, known_hbm, mu_hbm, chunk_ref, start_ref, known_ref, mu_ref, sems):
    copies = [
        pltpu.make_async_copy(src, dst, sems.at[n])
        for n, (src, dst) in enumerate(((start_hbm, start_ref), (known_hbm, known_ref), (mu_hbm, mu_ref)))
    ]
    for copy in copies:
        copy.start()
    for copy in copies:
        copy.wait()
    tile = planes_of(start_ref, known_ref, mu_ref)
    lane = lanes_of(8)
    zero = jnp.zeros((8, 128), F32)
    for j in range(16):
        side = zero
        for p in range(7):
            left = tile(p, 2 * j - 1) if j else zero
            right = tile(p, 2 * j + 2) if j < 15 else zero
            both = jnp.where(lane >= 125, left, right)
            side = jnp.where((lane >= 6 * p) & (lane < 6 * p + 6), turn(both, 6 * p + 3), side)
            for m in range(2):
                chunk_ref[j, pl.ds((2 * p + m) * 8, 8), :] = tile(p, 2 * j + m)
        chunk_ref[j, pl.ds(112, 8), :] = side


def beside(x, p):
    lane = lanes_of(x.shape[0])
    return jnp.where((lane < 3) | (lane >= 125), turn(x, 125 - 6 * p), 0.0)


def split3(x):
    a = x.astype(BF16)
    r = x - a.astype(F32)
    b = r.astype(BF16)
    return a, b, (r - b.astype(F32)).astype(BF16)


def permuted(x, table):
    a, b, c = split3(x)
    dot = lambda v: jnp.dot(v, table, preferred_element_type=F32)
    return dot(a) + dot(b) + dot(c)


def parity_table(forward, value=1.0):
    one = lax.broadcasted_iota(jnp.int32, (256, 256), 0 if forward else 1)
    two = lax.broadcasted_iota(jnp.int32, (256, 256), 1 if forward else 0)
    place = jnp.where(two < 128, 2 * two, 2 * two - 255)
    return jnp.where(one == place, value, 0.0).astype(BF16)


def fine_kernel(
    start_hbm, known_hbm, mu_hbm, fs_hbm, fk_hbm, fm_hbm, low_ref, high_ref, top_ref, bottom_ref,
    block, planes, sems, out_sems,
):
    copies = []
    for k in range(7):
        source = (start_hbm.at[k] if k < 3 else None, known_hbm.at[k - 3] if 3 <= k < 6 else None, mu_hbm)[
            0 if k < 3 else 1 if k < 6 else 2
        ]
        for c in range(4):
            n = 4 * k + c
            copies.append(pltpu.make_async_copy(source.at[:, pl.ds(128 * c, 128)], block.at[k, c], sems.at[n]))
    for copy in copies:
        copy.start()
    tables = parity_table(True), parity_table(True, 4.0)
    lane = lanes_of(PR)
    low_ref[...] = jnp.zeros((PR, 128), F32)
    high_ref[...] = jnp.zeros((PR, 128), F32)

    def put(ref, mask, value):
        ref[...] = jnp.where(mask, value, ref[...])

    written = []
    for k in range(7):
        for copy in copies[4 * k : 4 * k + 4]:
            copy.wait()
        out, t0 = (fs_hbm, fk_hbm, fm_hbm)[k // 3], 4 * k - 12 * (k // 3)
        for p in range(2):
            rows = pl.ds(p, PR, stride=2)
            for m in range(2):
                x = jnp.concatenate([block[k, 2 * m + c, rows, :] for c in range(2)], axis=1)
                y = permuted(x, tables[k >= 3])
                for q in range(2):
                    t = t0 + 2 * p + q
                    v = y[:, 128 * q : 128 * q + 128]
                    planes[4 * k + 2 * p + q, m, :, :] = v
                    if k < 3:
                        top_ref[m, pl.ds(2 * t, 2), :] = v[0:2]
                        bottom_ref[m, pl.ds(2 * t, 2), :] = v[126:128]
                        if m == 0:
                            put(low_ref, (lane == 4 * t + 2) | (lane == 4 * t + 3), turn(v, 4 * t + 2))
                        else:
                            put(high_ref, (lane == 4 * t) | (lane == 4 * t + 1), turn(v, 4 * t - 126))
                    else:
                        row, at = (24 + t, 48 + 2 * t) if k < 6 else (36 + t, 72 + 2 * t)
                        top_ref[m, pl.ds(row, 1), :] = v[0:1]
                        bottom_ref[m, pl.ds(row, 1), :] = v[127:128]
                        if m == 0:
                            put(low_ref, lane == at + 1, turn(v, at + 1))
                        else:
                            put(high_ref, lane == at, turn(v, at - 127))
        written.append(pltpu.make_async_copy(planes.at[pl.ds(4 * k, 4)], out.at[pl.ds(t0, 4)], out_sems.at[k]))
        written[-1].start()
    for copy in written:
        copy.wait()


def start_side(x, t):
    lane = lanes_of(x.shape[0])
    return jnp.where((lane < 2) | (lane >= 126), turn(x, 126 - 4 * t), 0.0)


def other_side(x, at):
    lane = lanes_of(x.shape[0])
    return jnp.where((lane < 1) | (lane >= 127), turn(x, 127 - at), 0.0)


def rows_kernel(left_ref, right_ref, top_ref, bottom_ref, first_ref, last_ref, up_ref, down_ref):
    for part, patch, out, two, one in ((top_ref, first_ref, up_ref, 0, 0), (bottom_ref, last_ref, down_ref, 126, 127)):
        out[0:2, 0:40, :] = part[...]
        pair = left_ref[two : two + 2] + right_ref[two : two + 2]
        single = left_ref[one : one + 1] + right_ref[one : one + 1]
        for t in range(12):
            out[2, pl.ds(2 * t, 2), :] = start_side(pair, t)
            out[2, pl.ds(24 + t, 1), :] = other_side(single, 48 + 2 * t)
        for t in range(4):
            out[2, pl.ds(36 + t, 1), :] = other_side(single, 72 + 2 * t)
        for p in range(7):
            row, count = edge_rows(p)
            at = 0 if one == 0 else 8 - count
            for m in range(2):
                out[m, pl.ds(row, count), :] = patch[0, pl.ds((2 * p + m) * 8 + at, count), :]
            out[2, pl.ds(row, count), :] = beside(patch[0, pl.ds(112 + at, count), :], p)


def sweep_kernel(
    fs_hbm, fk_hbm, fm_hbm, recv_ref, left_ref, right_ref, above_ref, below_ref,
    chunk_ref, fine_ref,
    ca, cb, xa, xb, kc, mc, rc, fa, fb, kf, mf, rf, sems,
):
    own = pl.ds(TOP, PR)
    copies = [
        pltpu.make_async_copy(src, dst.at[:, pl.ds(0, 2), own, :], sems.at[n])
        for n, (src, dst) in enumerate(((fm_hbm, mf), (fs_hbm, fa), (fk_hbm, kf)))
    ]
    for copy in copies:
        copy.start()
    zero8 = jnp.zeros((8, 128), F32)
    for ref, count in ((ca, 3), (kc, 3), (fa, 12), (kf, 12), (mf, 4)):
        for t in range(count):
            for m in range(3):
                for r in (TOP - 8, TOP + PR):
                    ref[t, m, pl.ds(r, 8), :] = zero8
    for m in range(3):
        for r in (TOP - 8, TOP + PR):
            mc[m, pl.ds(r, 8), :] = zero8
    lane8 = lanes_of(8)

    def coarse(p):
        return (ca.at[p], kc.at[p - 3] if 3 <= p < 6 else None, mc)[0 if p < 3 else 1 if p < 6 else 2]

    for p in range(7):
        ref = coarse(p)
        for j in range(16):
            rows = pl.ds(TOP + 8 * j, 8)
            for m in range(2):
                ref[m, rows, :] = recv_ref[j, pl.ds((2 * p + m) * 8, 8), :]
            ref[2, rows, :] = beside(recv_ref[j, pl.ds(112, 8), :], p)
        row, count = edge_rows(p)
        for m in range(3):
            ref[m, pl.ds(TOP - count, count), :] = above_ref[m, pl.ds(row, count), :]
            ref[m, pl.ds(TOP + PR, count), :] = below_ref[m, pl.ds(row, count), :]
    both = left_ref[...] + right_ref[...]
    for t in range(12):
        fa[t, 2, own, :] = start_side(both, t)
        kf[t, 2, own, :] = other_side(both, 48 + 2 * t)
    for t in range(4):
        mf[t, 2, own, :] = other_side(both, 72 + 2 * t)
    for m in range(3):
        for t in range(12):
            fa[t, m, pl.ds(TOP - 2, 2), :] = above_ref[m, pl.ds(2 * t, 2), :]
            fa[t, m, pl.ds(TOP + PR, 2), :] = below_ref[m, pl.ds(2 * t, 2), :]
            kf[t, m, pl.ds(TOP - 1, 1), :] = above_ref[m, pl.ds(24 + t, 1), :]
            kf[t, m, pl.ds(TOP + PR, 1), :] = below_ref[m, pl.ds(24 + t, 1), :]
        for t in range(4):
            mf[t, m, pl.ds(TOP - 1, 1), :] = above_ref[m, pl.ds(36 + t, 1), :]
            mf[t, m, pl.ds(TOP + PR, 1), :] = below_ref[m, pl.ds(36 + t, 1), :]
    copies[0].wait()

    at_start, at_end = lane8 == 0, lane8 == 127

    def before(x):
        turned = [turn(v, 1) for v in x]
        return [jnp.where(at_start, turned[m - 1], turned[m]) for m in range(len(x))]

    def after(x):
        turned = [turn(v, 127) for v in x]
        return [jnp.where(at_end, turned[(m + 1) % 3], turned[m]) for m in range(3)]

    def mix(x, k, r, c):
        west, east = before(c), after(c)
        for m in range(3):
            part = 0.375 * c[m]
            x[0, k, m, r, :] = part + 0.125 * west[m]
            x[1, k, m, r, :] = part + 0.125 * east[m]
            x[2, k, m, r, :] = west[m] + east[m]

    def ready(i, carry):
        r = pl.ds(pl.multiple_of(8 + 8 * i, 8), 8)
        for m in range(3):
            mu = mc[m, r, :]
            mc[m, r, :] = mu + 4.0
            rc[m, r, :] = jnp.where(mu > 0.0, 1.0 / (mu + 4.0), 0.0)
            for t in range(4):
                mu = mf[t, m, r, :]
                mf[t, m, r, :] = mu + 4.0
                rf[t, m, r, :] = jnp.where(mu > 0.0, 1.0 / (mu + 4.0), 0.0)
        for k in range(3):
            mix(xa, k, r, [ca[k, m, r, :] for m in range(3)])
        return carry

    lax.fori_loop(0, PR // 8 + 2, ready, 0, unroll=6)
    for copy in copies[1:]:
        copy.wait()

    def step(r, c_old, x_old, f_old, store_c, store_f, tiles, sums):
        here, up, down = pl.ds(r, 8), pl.ds(r - 1, 8), pl.ds(r + 1, 8)
        totals = [zero8] * 4
        for k in range(3):
            f = [[[f_old[4 * k + 2 * p + q, m, here, :] for m in range(3)] for q in range(2)] for p in range(2)]
            far = [[(before, after)[q](f[p][1 - q]) for q in range(2)] for p in range(2)]
            new = []
            for m in range(tiles):
                for q in range(2):
                    mid = 3.0 * x_old[q, k, m, here, :]
                    for p in range(2):
                        t, side = 4 * k + 2 * p + q, (up, down)[p]
                        other = f_old[4 * k + 2 * (1 - p) + q, m, side, :]
                        near = (f[1 - p][q][m] + other) + (f[p][1 - q][m] + far[p][q][m])
                        s = (kf[t, m, here, :] + near) + (mid + x_old[q, k, m, side, :])
                        store_f(t, m, s * rf[2 * p + q, m, here, :])
                        if sums and m < 2:
                            res = s - mf[2 * p + q, m, here, :] * f[p][q][m]
                            totals[2 * p + q] = totals[2 * p + q] + res * res
                c = c_old[k, m, here, :]
                near = (c_old[k, m, up, :] + c_old[k, m, down, :]) + x_old[2, k, m, here, :]
                four = (f[0][0][m] + f[0][1][m]) + (f[1][0][m] + f[1][1][m])
                s = (kc[k, m, here, :] + 0.5 * four) + near
                new.append(s * rc[m, here, :])
                if sums and m < 2:
                    res = s - mc[m, here, :] * c
                    totals[k] = totals[k] + res * res
            store_c(k, new)
        return (totals[0] + totals[1]) + (totals[2] + totals[3])

    def sweep(c_old, x_old, f_old, c_new, x_new, f_new):
        def stores(r):
            rows = pl.ds(r, 8)

            def store_c(k, new):
                for m in range(3):
                    c_new[k, m, rows, :] = new[m]
                mix(x_new, k, rows, new)

            def store_f(t, m, v):
                f_new[t, m, rows, :] = v

            return store_c, store_f

        def body(i, total):
            r = pl.multiple_of(TOP + 8 * i, 8)
            return total + step(r, c_old, x_old, f_old, *stores(r), 3, True)

        total = lax.fori_loop(0, PR // 8, body, zero8, unroll=4)

        def edge(i, carry):
            r = pl.multiple_of(TOP - 8 + i * (PR + 8), 8)
            step(r, c_old, x_old, f_old, *stores(r), 3, False)
            return carry

        lax.fori_loop(0, 2, edge, 0, unroll=True)
        return total

    totals = [sweep(ca, xa, fa, cb, xb, fb), sweep(cb, xb, fb, ca, xa, fa)]

    def last(i, total):
        r = pl.multiple_of(TOP + 8 * i, 8)

        def store_c(k, new):
            for m in range(2):
                chunk_ref[i, pl.ds((2 * k + m) * 8, 8), :] = new[m]

        def store_f(t, m, v):
            fine_ref[t, m, pl.ds(pl.multiple_of(8 * i, 8), 8), :] = v

        return total + step(r, ca, xa, fa, store_c, store_f, 2, True)

    totals.append(lax.fori_loop(0, PR // 8, last, zero8, unroll=4))
    sums = 0.0625 * jnp.concatenate([jnp.sum(v, axis=0, keepdims=True) for v in totals] + [jnp.zeros((5, 128), F32)], axis=0)
    for j in range(16):
        chunk_ref[j, pl.ds(48, 8), :] = sums


def join_kernel(fine_ref, out_hbm, block, sems):
    table = parity_table(False)
    copies = []
    for k in range(3):
        for m in range(2):
            for p in range(2):
                x = jnp.concatenate([fine_ref[4 * k + 2 * p + q, m, :, :] for q in range(2)], axis=1)
                y = permuted(x, table)
                for c in range(2):
                    block[k, 2 * m + c, pl.ds(p, PR, stride=2), :] = y[:, 128 * c : 128 * c + 128]
            for c in range(2 * m, 2 * m + 2):
                copy = pltpu.make_async_copy(
                    block.at[k, c], out_hbm.at[k, :, pl.ds(128 * c, 128)], sems.at[4 * k + c]
                )
                copy.start()
                copies.append(copy)
    for copy in copies:
        copy.wait()


def sum_kernel(recv_ref, out_ref):
    total = recv_ref[0]
    for j in range(1, 16):
        total = total + recv_ref[j]
    for i in range(8):
        out_ref[i] = total


def coarse_kernel(recv_ref, out_ref):
    for j in range(16):
        for k in range(3):
            for m in range(2):
                out_ref[k, :, pl.ds(256 * j + 128 * m, 128)] = recv_ref[j, pl.ds((2 * k + m) * 8, 8), :]


def on_device(fine_start, fine_known, fine_mu, coarse_start, coarse_known, coarse_mu):
    count_x, count_y = lax.axis_size(GX), lax.axis_size(GY)
    cell_total = 3.0 * (fine_mu.size + coarse_mu.size) * (count_x * count_y)
    chunk = pl.pallas_call(
        pack_kernel,
        out_shape=pltpu.VMEM((16, MAIN, 128), F32),
        in_specs=[HBM] * 3,
        out_specs=VMEM,
        scratch_shapes=[
            pltpu.VMEM(coarse_start.shape, F32),
            pltpu.VMEM(coarse_known.shape, F32),
            pltpu.VMEM(coarse_mu.shape, F32),
            pltpu.SemaphoreType.DMA((3,)),
        ],
        compiler_params=params(GRANT_KIB),
        cost_estimate=cost(2, 2e6),
        name="pack",
    )(*in_hbm(coarse_start, coarse_known, coarse_mu))
    recv = lax.all_to_all(chunk, GY, 0, 0, tiled=True)

    fs, fk, fm, low, high, top, bottom = pl.pallas_call(
        fine_kernel,
        out_shape=(
            *(pltpu.HBM((n, 2, PR, 128), F32) for n in (12, 12, 4)),
            *(pltpu.VMEM(shape, F32) for shape in ((PR, 128), (PR, 128), (2, 40, 128), (2, 40, 128))),
        ),
        in_specs=[HBM] * 3,
        out_specs=(HBM,) * 3 + (VMEM,) * 4,
        scratch_shapes=[
            pltpu.VMEM((7, 4, 2 * PR, 128), F32),
            pltpu.VMEM((28, 2, PR, 128), F32),
            pltpu.SemaphoreType.DMA((28,)),
            pltpu.SemaphoreType.DMA((7,)),
        ],
        compiler_params=params(GRANT_KIB),
        cost_estimate=cost(4, 7e6),
        name="fine",
    )(*in_hbm(fine_start, fine_known, fine_mu))

    def ahead(n):
        return [(i, i + 1) for i in range(n - 1)]

    def back(n):
        return [(i + 1, i) for i in range(n - 1)]

    left = lax.ppermute(high, GY, ahead(count_y))
    right = lax.ppermute(low, GY, back(count_y))
    up, down = pl.pallas_call(
        rows_kernel,
        grid=(1,),
        out_shape=(shaped(3, EDGE, 128),) * 2,
        in_specs=[pl.BlockSpec((PR, 128), lambda i: (0, 0))] * 2
        + [pl.BlockSpec((2, 40, 128), lambda i: (0, 0, 0))] * 2
        + [pl.BlockSpec((1, MAIN, 128), lambda i: (0, 0, 0)), pl.BlockSpec((1, MAIN, 128), lambda i: (15, 0, 0))],
        out_specs=(pl.BlockSpec((3, EDGE, 128), lambda i: (0, 0, 0)),) * 2,
        compiler_params=params(GRANT_KIB),
        cost_estimate=cost(1, 0.3e6),
        name="rows",
    )(left, right, top, bottom, recv, recv)
    above = lax.ppermute(down, GX, ahead(count_x))
    below = lax.ppermute(up, GX, back(count_x))

    chunk, fine = pl.pallas_call(
        sweep_kernel,
        out_shape=(pltpu.VMEM((16, 56, 128), F32), pltpu.VMEM((12, 2, PR, 128), F32)),
        in_specs=[HBM] * 3 + [VMEM] * 5,
        out_specs=(VMEM, VMEM),
        scratch_shapes=[
            pltpu.VMEM((3, 3, ROWS, 128), F32),
            pltpu.VMEM((3, 3, ROWS, 128), F32),
            pltpu.VMEM((3, 3, 3, ROWS, 128), F32),
            pltpu.VMEM((3, 3, 3, ROWS, 128), F32),
            pltpu.VMEM((3, 3, ROWS, 128), F32),
            pltpu.VMEM((3, ROWS, 128), F32),
            pltpu.VMEM((3, ROWS, 128), F32),
            pltpu.VMEM((12, 3, ROWS, 128), F32),
            pltpu.VMEM((12, 3, ROWS, 128), F32),
            pltpu.VMEM((12, 3, ROWS, 128), F32),
            pltpu.VMEM((4, 3, ROWS, 128), F32),
            pltpu.VMEM((4, 3, ROWS, 128), F32),
            pltpu.SemaphoreType.DMA((3,)),
        ],
        compiler_params=params(GRANT_KIB),
        cost_estimate=cost(8, 7e6),
        name="sweeps",
    )(*in_hbm(fs, fk, fm), recv, left, right, above, below)
    out = lax.all_to_all(chunk, GY, 0, 0, tiled=True)

    fine_ghost = pl.pallas_call(
        join_kernel,
        out_shape=shaped(*fine_start.shape),
        in_specs=[VMEM],
        out_specs=HBM,
        scratch_shapes=[
            pltpu.VMEM((3, 4, 2 * PR, 128), F32),
            pltpu.SemaphoreType.DMA((12,)),
        ],
        compiler_params=params(GRANT_KIB),
        cost_estimate=cost(2, 3e6),
        name="join",
    )(fine)
    sums = pl.pallas_call(
        sum_kernel,
        grid=(1,),
        out_shape=pltpu.VMEM((8, 8, 128), F32),
        in_specs=[pl.BlockSpec((16, 8, 128), lambda i: (0, 6, 0))],
        out_specs=pl.BlockSpec((8, 8, 128), lambda i: (0, 0, 0)),
        compiler_params=params(GRANT_KIB),
        cost_estimate=cost(1, 0.1e6),
        name="sums",
    )(out)
    sums = lax.all_to_all(sums, GX, 0, 0, tiled=True)
    coarse_ghost = pl.pallas_call(
        coarse_kernel,
        out_shape=shaped(*coarse_start.shape),
        in_specs=[VMEM],
        out_specs=VMEM,
        compiler_params=params(GRANT_KIB),
        cost_estimate=cost(1, 0.8e6),
        name="coarse",
    )(out)
    norms = jnp.sqrt(jnp.sum(sums[:, :ITERS, :], axis=(0, 2)) / cell_total)
    return fine_ghost, coarse_ghost, norms


def solution(mesh):
    fine, coarse = P(None, GX, GY), P(None, BOTH, None)
    return jax.shard_map(
        on_device,
        mesh=mesh,
        in_specs=(fine, fine, P(GX, GY), coarse, coarse, P(BOTH, None)),
        out_specs=(fine, coarse, P()),
        check_vma=False,
    )
```

```python
import jax
import jax.numpy as jnp
from jax import lax
from jax.experimental import pallas as pl
from jax.experimental.pallas import tpu as pltpu
from jax.sharding import PartitionSpec as P

ITERS = 3
GX, GY = "gx", "gy"
BOTH = (GX, GY)
PR = 128
TOP = 16
SPLIT = 64
ROWS = PR + 40
F32 = jnp.float32
BF16 = jnp.bfloat16
VMEM = pl.BlockSpec(memory_space=pltpu.VMEM)
HBM = pl.BlockSpec(memory_space=pltpu.HBM)


def shaped(*shape):
    return jax.ShapeDtypeStruct(shape, F32)


GRANT_KIB = 36864


def params(kib):
    return pltpu.CompilerParams(vmem_limit_bytes=kib << 10)


def cost(us, moved):
    return pl.CostEstimate(flops=int(us * 7.0e6), bytes_accessed=int(moved), transcendentals=0)


def in_hbm(*arrays):
    return tuple(pltpu.with_memory_space_constraint(a, pltpu.HBM) for a in arrays)


def lanes_of(rows):
    return lax.broadcasted_iota(jnp.int32, (rows, 128), 1)


def turn(x, shift):
    shift %= 128
    return x if shift == 0 else pltpu.roll(x, shift, axis=1)


MAIN = 120
EDGE = 64


def edge_rows(p):
    return (40 + 3 * p, 3) if p < 3 else (43 + 2 * p, 2)


def planes_of(start_ref, known_ref, mu_ref):
    def tile(p, t):
        cols = pl.ds(128 * t, 128)
        if p < 3:
            return start_ref[p, :, cols]
        if p < 6:
            return 4.0 * known_ref[p - 3, :, cols]
        return 4.0 * mu_ref[:, cols]

    return tile


def pack_kernel(start_hbm, known_hbm, mu_hbm, chunk_hbm, start_ref, known_ref, mu_ref, chunk_ref, sems, out_sems):
    width = start_ref.shape[-1] // 4
    reads, writes = [], []
    for n in range(4):
        cols = pl.ds(n * width, width)
        for i, (src, dst) in enumerate(((start_hbm, start_ref), (known_hbm, known_ref))):
            reads.append(pltpu.make_async_copy(src.at[:, :, cols], dst.at[:, :, cols], sems.at[3 * n + i]))
        reads.append(pltpu.make_async_copy(mu_hbm.at[:, cols], mu_ref.at[:, cols], sems.at[3 * n + 2]))
    for copy in reads:
        copy.start()
    for copy in reads[:3]:
        copy.wait()
    tile = planes_of(start_ref, known_ref, mu_ref)
    lane = lanes_of(8)
    zero = jnp.zeros((8, 128), F32)
    for j in range(16):
        n = j // 4
        if j % 4 == 3 and n < 3:
            for copy in reads[3 * n + 3 : 3 * n + 6]:
                copy.wait()
        side = zero
        for p in range(7):
            left = tile(p, 2 * j - 1) if j else zero
            right = tile(p, 2 * j + 2) if j < 15 else zero
            both = jnp.where(lane >= 125, left, right)
            side = jnp.where((lane >= 6 * p) & (lane < 6 * p + 6), turn(both, 6 * p + 3), side)
            for m in range(2):
                chunk_ref[j, pl.ds((2 * p + m) * 8, 8), :] = tile(p, 2 * j + m)
        chunk_ref[j, pl.ds(112, 8), :] = side
        if j % 4 == 3:
            group = pl.ds(4 * n, 4)
            writes.append(pltpu.make_async_copy(chunk_ref.at[group], chunk_hbm.at[group], out_sems.at[n]))
            writes[-1].start()
    for copy in writes:
        copy.wait()


def beside(x, p):
    lane = lanes_of(x.shape[0])
    return jnp.where((lane < 3) | (lane >= 125), turn(x, 125 - 6 * p), 0.0)


def split3(x):
    a = x.astype(BF16)
    r = x - a.astype(F32)
    b = r.astype(BF16)
    return a, b, (r - b.astype(F32)).astype(BF16)


def permuted(x, table):
    a, b, c = split3(x)
    dot = lambda v: jnp.dot(v, table, preferred_element_type=F32)
    return dot(a) + dot(b) + dot(c)


def parity_table(forward, value=1.0):
    one = lax.broadcasted_iota(jnp.int32, (256, 256), 0 if forward else 1)
    two = lax.broadcasted_iota(jnp.int32, (256, 256), 1 if forward else 0)
    place = jnp.where(two < 128, 2 * two, 2 * two - 255)
    return jnp.where(one == place, value, 0.0).astype(BF16)


def fine_kernel(
    start_hbm, known_hbm, mu_hbm, fs_hbm, fk_hbm, fm_hbm, low_ref, high_ref, top_ref, bottom_ref,
    block, planes, sems, out_sems,
):
    copies = []
    for k in range(7):
        source = (start_hbm.at[k] if k < 3 else None, known_hbm.at[k - 3] if 3 <= k < 6 else None, mu_hbm)[
            0 if k < 3 else 1 if k < 6 else 2
        ]
        for c in range(4):
            n = 4 * k + c
            copies.append(pltpu.make_async_copy(source.at[:, pl.ds(128 * c, 128)], block.at[k, c], sems.at[n]))
    for copy in copies:
        copy.start()
    tables = parity_table(True), parity_table(True, 4.0)
    lane = lanes_of(PR)
    low_ref[...] = jnp.zeros((PR, 128), F32)
    high_ref[...] = jnp.zeros((PR, 128), F32)

    def put(ref, mask, value):
        ref[...] = jnp.where(mask, value, ref[...])

    written = []
    for k in range(7):
        for copy in copies[4 * k : 4 * k + 4]:
            copy.wait()
        out, t0 = (fs_hbm, fk_hbm, fm_hbm)[k // 3], 4 * k - 12 * (k // 3)
        for p in range(2):
            rows = pl.ds(p, PR, stride=2)
            for m in range(2):
                x = jnp.concatenate([block[k, 2 * m + c, rows, :] for c in range(2)], axis=1)
                y = permuted(x, tables[k >= 3])
                for q in range(2):
                    t = t0 + 2 * p + q
                    v = y[:, 128 * q : 128 * q + 128]
                    planes[4 * k + 2 * p + q, m, :, :] = v
                    if k < 3:
                        top_ref[m, pl.ds(2 * t, 2), :] = v[0:2]
                        bottom_ref[m, pl.ds(2 * t, 2), :] = v[126:128]
                        if m == 0:
                            put(low_ref, (lane == 4 * t + 2) | (lane == 4 * t + 3), turn(v, 4 * t + 2))
                        else:
                            put(high_ref, (lane == 4 * t) | (lane == 4 * t + 1), turn(v, 4 * t - 126))
                    else:
                        row, at = (24 + t, 48 + 2 * t) if k < 6 else (36 + t, 72 + 2 * t)
                        top_ref[m, pl.ds(row, 1), :] = v[0:1]
                        bottom_ref[m, pl.ds(row, 1), :] = v[127:128]
                        if m == 0:
                            put(low_ref, lane == at + 1, turn(v, at + 1))
                        else:
                            put(high_ref, lane == at, turn(v, at - 127))
        written.append(pltpu.make_async_copy(planes.at[pl.ds(4 * k, 4)], out.at[pl.ds(t0, 4)], out_sems.at[k]))
        written[-1].start()
    for copy in written:
        copy.wait()


def start_side(x, t):
    lane = lanes_of(x.shape[0])
    return jnp.where((lane < 2) | (lane >= 126), turn(x, 126 - 4 * t), 0.0)


def other_side(x, at):
    lane = lanes_of(x.shape[0])
    return jnp.where((lane < 1) | (lane >= 127), turn(x, 127 - at), 0.0)


def rows_kernel(left_ref, right_ref, top_ref, bottom_ref, first_ref, last_ref, up_ref, down_ref):
    for part, patch, out, two, one in ((top_ref, first_ref, up_ref, 0, 0), (bottom_ref, last_ref, down_ref, 126, 127)):
        out[0:2, 0:40, :] = part[...]
        pair = left_ref[two : two + 2] + right_ref[two : two + 2]
        single = left_ref[one : one + 1] + right_ref[one : one + 1]
        for t in range(12):
            out[2, pl.ds(2 * t, 2), :] = start_side(pair, t)
            out[2, pl.ds(24 + t, 1), :] = other_side(single, 48 + 2 * t)
        for t in range(4):
            out[2, pl.ds(36 + t, 1), :] = other_side(single, 72 + 2 * t)
        for p in range(7):
            row, count = edge_rows(p)
            at = 0 if one == 0 else 8 - count
            for m in range(2):
                out[m, pl.ds(row, count), :] = patch[0, pl.ds((2 * p + m) * 8 + at, count), :]
            out[2, pl.ds(row, count), :] = beside(patch[0, pl.ds(112 + at, count), :], p)


def sweep_kernel(
    fs_hbm, fk_hbm, fm_hbm, recv_ref, left_ref, right_ref, above_ref, below_ref,
    chunk_ref, fine_ref,
    ca, cb, xa, xb, kc, mc, rc, fa, fb, kf, mf, rf, sems,
):
    own = pl.ds(TOP, PR)
    copies = []
    for src, dst, first, last in (
        (fm_hbm, mf, 0, PR), (fs_hbm, fa, 0, SPLIT + 8), (fk_hbm, kf, 0, SPLIT),
        (fs_hbm, fa, SPLIT + 8, PR), (fk_hbm, kf, SPLIT, PR),
    ):
        rows, place = pl.ds(first, last - first), pl.ds(TOP + first, last - first)
        copies.append(
            pltpu.make_async_copy(src.at[:, :, rows, :], dst.at[:, pl.ds(0, 2), place, :], sems.at[len(copies)])
        )
    for copy in copies:
        copy.start()
    zero8 = jnp.zeros((8, 128), F32)
    for ref, count in ((ca, 3), (kc, 3), (fa, 12), (kf, 12), (mf, 4)):
        for t in range(count):
            for m in range(3):
                for r in (TOP - 8, TOP + PR):
                    ref[t, m, pl.ds(r, 8), :] = zero8
    for m in range(3):
        for r in (TOP - 8, TOP + PR):
            mc[m, pl.ds(r, 8), :] = zero8
    lane8 = lanes_of(8)

    def coarse(p):
        return (ca.at[p], kc.at[p - 3] if 3 <= p < 6 else None, mc)[0 if p < 3 else 1 if p < 6 else 2]

    for p in range(7):
        ref = coarse(p)
        for j in range(16):
            rows = pl.ds(TOP + 8 * j, 8)
            for m in range(2):
                ref[m, rows, :] = recv_ref[j, pl.ds((2 * p + m) * 8, 8), :]
            ref[2, rows, :] = beside(recv_ref[j, pl.ds(112, 8), :], p)
        row, count = edge_rows(p)
        for m in range(3):
            ref[m, pl.ds(TOP - count, count), :] = above_ref[m, pl.ds(row, count), :]
            ref[m, pl.ds(TOP + PR, count), :] = below_ref[m, pl.ds(row, count), :]
    both = left_ref[...] + right_ref[...]
    for t in range(12):
        fa[t, 2, own, :] = start_side(both, t)
        kf[t, 2, own, :] = other_side(both, 48 + 2 * t)
    for t in range(4):
        mf[t, 2, own, :] = other_side(both, 72 + 2 * t)
    for m in range(3):
        for t in range(12):
            fa[t, m, pl.ds(TOP - 2, 2), :] = above_ref[m, pl.ds(2 * t, 2), :]
            fa[t, m, pl.ds(TOP + PR, 2), :] = below_ref[m, pl.ds(2 * t, 2), :]
            kf[t, m, pl.ds(TOP - 1, 1), :] = above_ref[m, pl.ds(24 + t, 1), :]
            kf[t, m, pl.ds(TOP + PR, 1), :] = below_ref[m, pl.ds(24 + t, 1), :]
        for t in range(4):
            mf[t, m, pl.ds(TOP - 1, 1), :] = above_ref[m, pl.ds(36 + t, 1), :]
            mf[t, m, pl.ds(TOP + PR, 1), :] = below_ref[m, pl.ds(36 + t, 1), :]
    copies[0].wait()

    at_start, at_end = lane8 == 0, lane8 == 127

    def before(x):
        turned = [turn(v, 1) for v in x]
        return [jnp.where(at_start, turned[m - 1], turned[m]) for m in range(len(x))]

    def after(x):
        turned = [turn(v, 127) for v in x]
        return [jnp.where(at_end, turned[(m + 1) % 3], turned[m]) for m in range(3)]

    def mix(x, k, r, c):
        west, east = before(c), after(c)
        for m in range(3):
            part = 0.375 * c[m]
            x[0, k, m, r, :] = part + 0.125 * west[m]
            x[1, k, m, r, :] = part + 0.125 * east[m]
            x[2, k, m, r, :] = west[m] + east[m]

    def ready(i, carry):
        r = pl.ds(pl.multiple_of(8 + 8 * i, 8), 8)
        for m in range(3):
            mu = mc[m, r, :]
            mc[m, r, :] = mu + 4.0
            rc[m, r, :] = jnp.where(mu > 0.0, 1.0 / (mu + 4.0), 0.0)
            for t in range(4):
                mu = mf[t, m, r, :]
                mf[t, m, r, :] = mu + 4.0
                rf[t, m, r, :] = jnp.where(mu > 0.0, 1.0 / (mu + 4.0), 0.0)
        for k in range(3):
            mix(xa, k, r, [ca[k, m, r, :] for m in range(3)])
        return carry

    lax.fori_loop(0, PR // 8 + 2, ready, 0, unroll=9)
    for copy in copies[1:3]:
        copy.wait()

    def step(r, c_old, x_old, f_old, store_c, store_f, tiles, sums):
        here, up, down = pl.ds(r, 8), pl.ds(r - 1, 8), pl.ds(r + 1, 8)
        totals = [zero8] * 4
        for k in range(3):
            f = [[[f_old[4 * k + 2 * p + q, m, here, :] for m in range(3)] for q in range(2)] for p in range(2)]
            far = [[(before, after)[q](f[p][1 - q]) for q in range(2)] for p in range(2)]
            new = []
            for m in range(tiles):
                for q in range(2):
                    mid = 3.0 * x_old[q, k, m, here, :]
                    for p in range(2):
                        t, side = 4 * k + 2 * p + q, (up, down)[p]
                        other = f_old[4 * k + 2 * (1 - p) + q, m, side, :]
                        near = (f[1 - p][q][m] + other) + (f[p][1 - q][m] + far[p][q][m])
                        s = (kf[t, m, here, :] + near) + (mid + x_old[q, k, m, side, :])
                        store_f(t, m, s * rf[2 * p + q, m, here, :])
                        if sums and m < 2:
                            res = s - mf[2 * p + q, m, here, :] * f[p][q][m]
                            totals[2 * p + q] = totals[2 * p + q] + res * res
                c = c_old[k, m, here, :]
                near = (c_old[k, m, up, :] + c_old[k, m, down, :]) + x_old[2, k, m, here, :]
                four = (f[0][0][m] + f[0][1][m]) + (f[1][0][m] + f[1][1][m])
                s = (kc[k, m, here, :] + 0.5 * four) + near
                new.append(s * rc[m, here, :])
                if sums and m < 2:
                    res = s - mc[m, here, :] * c
                    totals[k] = totals[k] + res * res
            store_c(k, new)
        return (totals[0] + totals[1]) + (totals[2] + totals[3])

    def sweep(c_old, x_old, f_old, c_new, x_new, f_new, pending):
        def stores(r):
            rows = pl.ds(r, 8)

            def store_c(k, new):
                for m in range(3):
                    c_new[k, m, rows, :] = new[m]
                mix(x_new, k, rows, new)

            def store_f(t, m, v):
                f_new[t, m, rows, :] = v

            return store_c, store_f

        def body(i, total):
            r = pl.multiple_of(TOP + 8 * i, 8)
            return total + step(r, c_old, x_old, f_old, *stores(r), 3, True)

        half = SPLIT // 8
        total = lax.fori_loop(0, half, body, zero8, unroll=half)
        for copy in pending:
            copy.wait()
        total = lax.fori_loop(half, PR // 8, body, total, unroll=half)

        def edge(i, carry):
            r = pl.multiple_of(TOP - 8 + i * (PR + 8), 8)
            step(r, c_old, x_old, f_old, *stores(r), 3, False)
            return carry

        lax.fori_loop(0, 2, edge, 0, unroll=True)
        return total

    totals = [sweep(ca, xa, fa, cb, xb, fb, copies[3:]), sweep(cb, xb, fb, ca, xa, fa, [])]

    def last(i, total):
        r = pl.multiple_of(TOP + 8 * i, 8)

        def store_c(k, new):
            for m in range(2):
                chunk_ref[i, pl.ds((2 * k + m) * 8, 8), :] = new[m]

        def store_f(t, m, v):
            fine_ref[t, m, pl.ds(pl.multiple_of(8 * i, 8), 8), :] = v

        return total + step(r, ca, xa, fa, store_c, store_f, 2, True)

    totals.append(lax.fori_loop(0, PR // 8, last, zero8, unroll=8))
    sums = 0.0625 * jnp.concatenate([jnp.sum(v, axis=0, keepdims=True) for v in totals] + [jnp.zeros((5, 128), F32)], axis=0)
    for j in range(16):
        chunk_ref[j, pl.ds(48, 8), :] = sums


def join_kernel(fine_ref, out_hbm, block, sems):
    table = parity_table(False)
    copies = []
    for k in range(3):
        for m in range(2):
            for p in range(2):
                x = jnp.concatenate([fine_ref[4 * k + 2 * p + q, m, :, :] for q in range(2)], axis=1)
                y = permuted(x, table)
                for c in range(2):
                    block[k, 2 * m + c, pl.ds(p, PR, stride=2), :] = y[:, 128 * c : 128 * c + 128]
            for c in range(2 * m, 2 * m + 2):
                copy = pltpu.make_async_copy(
                    block.at[k, c], out_hbm.at[k, :, pl.ds(128 * c, 128)], sems.at[4 * k + c]
                )
                copy.start()
                copies.append(copy)
    for copy in copies:
        copy.wait()


def sum_kernel(recv_ref, out_ref):
    total = recv_ref[0]
    for j in range(1, 16):
        total = total + recv_ref[j]
    for i in range(8):
        out_ref[i] = total


def coarse_kernel(recv_ref, out_ref):
    for j in range(16):
        for k in range(3):
            for m in range(2):
                out_ref[k, :, pl.ds(256 * j + 128 * m, 128)] = recv_ref[j, pl.ds((2 * k + m) * 8, 8), :]


def on_device(fine_start, fine_known, fine_mu, coarse_start, coarse_known, coarse_mu):
    count_x, count_y = lax.axis_size(GX), lax.axis_size(GY)
    cell_total = 3.0 * (fine_mu.size + coarse_mu.size) * (count_x * count_y)
    chunk = pl.pallas_call(
        pack_kernel,
        out_shape=pltpu.HBM((16, MAIN, 128), F32),
        in_specs=[HBM] * 3,
        out_specs=HBM,
        scratch_shapes=[
            pltpu.VMEM(coarse_start.shape, F32),
            pltpu.VMEM(coarse_known.shape, F32),
            pltpu.VMEM(coarse_mu.shape, F32),
            pltpu.VMEM((16, MAIN, 128), F32),
            pltpu.SemaphoreType.DMA((12,)),
            pltpu.SemaphoreType.DMA((4,)),
        ],
        compiler_params=params(GRANT_KIB),
        cost_estimate=cost(2, 2e6),
        name="pack",
    )(*in_hbm(coarse_start, coarse_known, coarse_mu))
    recv = lax.all_to_all(chunk, GY, 0, 0, tiled=True)

    fs, fk, fm, low, high, top, bottom = pl.pallas_call(
        fine_kernel,
        out_shape=(
            *(pltpu.HBM((n, 2, PR, 128), F32) for n in (12, 12, 4)),
            *(pltpu.VMEM(shape, F32) for shape in ((PR, 128), (PR, 128), (2, 40, 128), (2, 40, 128))),
        ),
        in_specs=[HBM] * 3,
        out_specs=(HBM,) * 3 + (VMEM,) * 4,
        scratch_shapes=[
            pltpu.VMEM((7, 4, 2 * PR, 128), F32),
            pltpu.VMEM((28, 2, PR, 128), F32),
            pltpu.SemaphoreType.DMA((28,)),
            pltpu.SemaphoreType.DMA((7,)),
        ],
        compiler_params=params(GRANT_KIB),
        cost_estimate=cost(4, 7e6),
        name="fine",
    )(*in_hbm(fine_start, fine_known, fine_mu))

    def ahead(n):
        return [(i, i + 1) for i in range(n - 1)]

    def back(n):
        return [(i + 1, i) for i in range(n - 1)]

    left = lax.ppermute(high, GY, ahead(count_y))
    right = lax.ppermute(low, GY, back(count_y))
    up, down = pl.pallas_call(
        rows_kernel,
        grid=(1,),
        out_shape=(shaped(3, EDGE, 128),) * 2,
        in_specs=[pl.BlockSpec((PR, 128), lambda i: (0, 0))] * 2
        + [pl.BlockSpec((2, 40, 128), lambda i: (0, 0, 0))] * 2
        + [pl.BlockSpec((1, MAIN, 128), lambda i: (0, 0, 0)), pl.BlockSpec((1, MAIN, 128), lambda i: (15, 0, 0))],
        out_specs=(pl.BlockSpec((3, EDGE, 128), lambda i: (0, 0, 0)),) * 2,
        compiler_params=params(GRANT_KIB),
        cost_estimate=cost(1, 0.3e6),
        name="rows",
    )(left, right, top, bottom, recv, recv)
    above = lax.ppermute(down, GX, ahead(count_x))
    below = lax.ppermute(up, GX, back(count_x))

    chunk, fine = pl.pallas_call(
        sweep_kernel,
        out_shape=(pltpu.VMEM((16, 56, 128), F32), pltpu.VMEM((12, 2, PR, 128), F32)),
        in_specs=[HBM] * 3 + [VMEM] * 5,
        out_specs=(VMEM, VMEM),
        scratch_shapes=[
            pltpu.VMEM((3, 3, ROWS, 128), F32),
            pltpu.VMEM((3, 3, ROWS, 128), F32),
            pltpu.VMEM((3, 3, 3, ROWS, 128), F32),
            pltpu.VMEM((3, 3, 3, ROWS, 128), F32),
            pltpu.VMEM((3, 3, ROWS, 128), F32),
            pltpu.VMEM((3, ROWS, 128), F32),
            pltpu.VMEM((3, ROWS, 128), F32),
            pltpu.VMEM((12, 3, ROWS, 128), F32),
            pltpu.VMEM((12, 3, ROWS, 128), F32),
            pltpu.VMEM((12, 3, ROWS, 128), F32),
            pltpu.VMEM((4, 3, ROWS, 128), F32),
            pltpu.VMEM((4, 3, ROWS, 128), F32),
            pltpu.SemaphoreType.DMA((5,)),
        ],
        compiler_params=params(GRANT_KIB),
        cost_estimate=cost(8, 7e6),
        name="sweeps",
    )(*in_hbm(fs, fk, fm), recv, left, right, above, below)
    out = lax.all_to_all(chunk, GY, 0, 0, tiled=True)

    fine_ghost = pl.pallas_call(
        join_kernel,
        out_shape=shaped(*fine_start.shape),
        in_specs=[VMEM],
        out_specs=HBM,
        scratch_shapes=[
            pltpu.VMEM((3, 4, 2 * PR, 128), F32),
            pltpu.SemaphoreType.DMA((12,)),
        ],
        compiler_params=params(GRANT_KIB),
        cost_estimate=cost(2, 3e6),
        name="join",
    )(fine)
    sums = pl.pallas_call(
        sum_kernel,
        grid=(1,),
        out_shape=pltpu.VMEM((8, 8, 128), F32),
        in_specs=[pl.BlockSpec((16, 8, 128), lambda i: (0, 6, 0))],
        out_specs=pl.BlockSpec((8, 8, 128), lambda i: (0, 0, 0)),
        compiler_params=params(GRANT_KIB),
        cost_estimate=cost(1, 0.1e6),
        name="sums",
    )(out)
    sums = lax.all_to_all(sums, GX, 0, 0, tiled=True)
    coarse_ghost = pl.pallas_call(
        coarse_kernel,
        out_shape=shaped(*coarse_start.shape),
        in_specs=[VMEM],
        out_specs=VMEM,
        compiler_params=params(GRANT_KIB),
        cost_estimate=cost(1, 0.8e6),
        name="coarse",
    )(out)
    norms = jnp.sqrt(jnp.sum(sums[:, :ITERS, :], axis=(0, 2)) / cell_total)
    return fine_ghost, coarse_ghost, norms


def solution(mesh):
    fine, coarse = P(None, GX, GY), P(None, BOTH, None)
    return jax.shard_map(
        on_device,
        mesh=mesh,
        in_specs=(fine, fine, P(GX, GY), coarse, coarse, P(BOTH, None)),
        out_specs=(fine, coarse, P()),
        check_vma=False,
    )
```

```python
import jax
import jax.numpy as jnp
from jax import lax
from jax.experimental import pallas as pl
from jax.experimental.pallas import tpu as pltpu
from jax.sharding import PartitionSpec as P

ITERS = 3
GX, GY = "gx", "gy"
BOTH = (GX, GY)
PR = 128
TOP = 16
SPLIT = 64
ROWS = PR + 40
F32 = jnp.float32
BF16 = jnp.bfloat16
VMEM = pl.BlockSpec(memory_space=pltpu.VMEM)
HBM = pl.BlockSpec(memory_space=pltpu.HBM)


def shaped(*shape):
    return jax.ShapeDtypeStruct(shape, F32)


GRANT_KIB = 36864


def params(kib):
    return pltpu.CompilerParams(vmem_limit_bytes=kib << 10)


def cost(us, moved):
    return pl.CostEstimate(flops=int(us * 7.0e6), bytes_accessed=int(moved), transcendentals=0)


def in_hbm(*arrays):
    return tuple(pltpu.with_memory_space_constraint(a, pltpu.HBM) for a in arrays)


def lanes_of(rows):
    return lax.broadcasted_iota(jnp.int32, (rows, 128), 1)


def turn(x, shift):
    shift %= 128
    return x if shift == 0 else pltpu.roll(x, shift, axis=1)


MAIN = 120
TILE_ROWS = 57
PAIR, SIDE, EDGE = 2 * TILE_ROWS, 2 * TILE_ROWS + 2, 120


def edge_rows(p):
    return (40 + 3 * p, 3) if p < 3 else (43 + 2 * p, 2)


def planes_of(start_ref, known_ref, mu_ref):
    def tile(p, t):
        cols = pl.ds(128 * t, 128)
        if p < 3:
            return start_ref[p, :, cols]
        if p < 6:
            return 4.0 * known_ref[p - 3, :, cols]
        return 4.0 * mu_ref[:, cols]

    return tile


def pack_kernel(start_hbm, known_hbm, mu_hbm, chunk_hbm, start_ref, known_ref, mu_ref, chunk_ref, sems, out_sems):
    width = start_ref.shape[-1] // 4
    reads, writes = [], []
    for n in range(4):
        cols = pl.ds(n * width, width)
        for i, (src, dst) in enumerate(((start_hbm, start_ref), (known_hbm, known_ref))):
            reads.append(pltpu.make_async_copy(src.at[:, :, cols], dst.at[:, :, cols], sems.at[3 * n + i]))
        reads.append(pltpu.make_async_copy(mu_hbm.at[:, cols], mu_ref.at[:, cols], sems.at[3 * n + 2]))
    for copy in reads:
        copy.start()
    for copy in reads[:3]:
        copy.wait()
    tile = planes_of(start_ref, known_ref, mu_ref)
    lane = lanes_of(8)
    zero = jnp.zeros((8, 128), F32)
    for j in range(16):
        n = j // 4
        if j % 4 == 3 and n < 3:
            for copy in reads[3 * n + 3 : 3 * n + 6]:
                copy.wait()
        side = zero
        for p in range(7):
            left = tile(p, 2 * j - 1) if j else zero
            right = tile(p, 2 * j + 2) if j < 15 else zero
            both = jnp.where(lane >= 125, left, right)
            side = jnp.where((lane >= 6 * p) & (lane < 6 * p + 6), turn(both, 6 * p + 3), side)
            for m in range(2):
                chunk_ref[j, pl.ds((2 * p + m) * 8, 8), :] = tile(p, 2 * j + m)
        chunk_ref[j, pl.ds(112, 8), :] = side
        if j % 4 == 3:
            group = pl.ds(4 * n, 4)
            writes.append(pltpu.make_async_copy(chunk_ref.at[group], chunk_hbm.at[group], out_sems.at[n]))
            writes[-1].start()
    for copy in writes:
        copy.wait()


def beside(x, p):
    lane = lanes_of(x.shape[0])
    return jnp.where((lane < 3) | (lane >= 125), turn(x, 125 - 6 * p), 0.0)


def split3(x):
    a = x.astype(BF16)
    r = x - a.astype(F32)
    b = r.astype(BF16)
    return a, b, (r - b.astype(F32)).astype(BF16)


def permuted(x, table):
    a, b, c = split3(x)
    dot = lambda v: jnp.dot(v, table, preferred_element_type=F32)
    return dot(a) + dot(b) + dot(c)


def parity_table(forward, value=1.0):
    one = lax.broadcasted_iota(jnp.int32, (256, 256), 0 if forward else 1)
    two = lax.broadcasted_iota(jnp.int32, (256, 256), 1 if forward else 0)
    place = jnp.where(two < 128, 2 * two, 2 * two - 255)
    return jnp.where(one == place, value, 0.0).astype(BF16)


def fine_kernel(
    start_hbm, known_hbm, mu_hbm, fs_hbm, fk_hbm, fm_hbm, low_ref, high_ref, top_ref, bottom_ref,
    block, planes, sems, out_sems,
):
    copies = []
    for k in range(7):
        source = (start_hbm.at[k] if k < 3 else None, known_hbm.at[k - 3] if 3 <= k < 6 else None, mu_hbm)[
            0 if k < 3 else 1 if k < 6 else 2
        ]
        for c in range(4):
            n = 4 * k + c
            copies.append(pltpu.make_async_copy(source.at[:, pl.ds(128 * c, 128)], block.at[k, c], sems.at[n]))
    for copy in copies:
        copy.start()
    tables = parity_table(True), parity_table(True, 4.0)
    lane = lanes_of(PR)
    low_ref[...] = jnp.zeros((PR, 128), F32)
    high_ref[...] = jnp.zeros((PR, 128), F32)

    def put(ref, mask, value):
        ref[...] = jnp.where(mask, value, ref[...])

    written = []
    for k in range(7):
        for copy in copies[4 * k : 4 * k + 4]:
            copy.wait()
        out, t0 = (fs_hbm, fk_hbm, fm_hbm)[k // 3], 4 * k - 12 * (k // 3)
        for p in range(2):
            rows = pl.ds(p, PR, stride=2)
            for m in range(2):
                x = jnp.concatenate([block[k, 2 * m + c, rows, :] for c in range(2)], axis=1)
                y = permuted(x, tables[k >= 3])
                for q in range(2):
                    t = t0 + 2 * p + q
                    v = y[:, 128 * q : 128 * q + 128]
                    planes[4 * k + 2 * p + q, m, :, :] = v
                    if k < 3:
                        top_ref[m, pl.ds(2 * t, 2), :] = v[0:2]
                        bottom_ref[m, pl.ds(2 * t, 2), :] = v[126:128]
                        if m == 0:
                            put(low_ref, (lane == 4 * t + 2) | (lane == 4 * t + 3), turn(v, 4 * t + 2))
                        else:
                            put(high_ref, (lane == 4 * t) | (lane == 4 * t + 1), turn(v, 4 * t - 126))
                    else:
                        row, at = (24 + t, 48 + 2 * t) if k < 6 else (36 + t, 72 + 2 * t)
                        top_ref[m, pl.ds(row, 1), :] = v[0:1]
                        bottom_ref[m, pl.ds(row, 1), :] = v[127:128]
                        if m == 0:
                            put(low_ref, lane == at + 1, turn(v, at + 1))
                        else:
                            put(high_ref, lane == at, turn(v, at - 127))
        written.append(pltpu.make_async_copy(planes.at[pl.ds(4 * k, 4)], out.at[pl.ds(t0, 4)], out_sems.at[k]))
        written[-1].start()
    for copy in written:
        copy.wait()


def start_side(x, t):
    lane = lanes_of(x.shape[0])
    return jnp.where((lane < 2) | (lane >= 126), turn(x, 126 - 4 * t), 0.0)


def other_side(x, at):
    lane = lanes_of(x.shape[0])
    return jnp.where((lane < 1) | (lane >= 127), turn(x, 127 - at), 0.0)


def rows_kernel(left_ref, right_ref, top_ref, bottom_ref, first_ref, last_ref, up_ref, down_ref):
    for part, patch, out, low in ((top_ref, first_ref, up_ref, True), (bottom_ref, last_ref, down_ref, False)):
        two = 0 if low else PR - 2
        for m in range(2):
            out[pl.ds(m * TILE_ROWS, 40), :] = part[m]
            for p in range(7):
                row, count = edge_rows(p)
                at = (2 * p + m) * 8 + (0 if low else 8 - count)
                out[pl.ds(m * TILE_ROWS + row, count), :] = patch[0, pl.ds(at, count), :]
        out[pl.ds(PAIR, 2), :] = left_ref[two : two + 2] + right_ref[two : two + 2]
        out[pl.ds(SIDE, 3), :] = patch[0, pl.ds(112 if low else 117, 3), :]
        out[pl.ds(SIDE + 3, 1), :] = jnp.zeros((1, 128), F32)


def sweep_kernel(
    fs_hbm, fk_hbm, fm_hbm, recv_ref, left_ref, right_ref, above_ref, below_ref,
    chunk_ref, fine_ref,
    ca, cb, xa, xb, kc, mc, rc, fa, fb, kf, mf, rf, sems,
):
    own = pl.ds(TOP, PR)
    copies = []
    for src, dst, first, last in (
        (fm_hbm, mf, 0, PR), (fs_hbm, fa, 0, SPLIT + 8), (fk_hbm, kf, 0, SPLIT),
        (fs_hbm, fa, SPLIT + 8, PR), (fk_hbm, kf, SPLIT, PR),
    ):
        rows, place = pl.ds(first, last - first), pl.ds(TOP + first, last - first)
        copies.append(
            pltpu.make_async_copy(src.at[:, :, rows, :], dst.at[:, pl.ds(0, 2), place, :], sems.at[len(copies)])
        )
    for copy in copies:
        copy.start()
    zero8 = jnp.zeros((8, 128), F32)
    for ref, count in ((ca, 3), (kc, 3), (fa, 12), (kf, 12), (mf, 4)):
        for t in range(count):
            for m in range(3):
                for r in (TOP - 8, TOP + PR):
                    ref[t, m, pl.ds(r, 8), :] = zero8
    for m in range(3):
        for r in (TOP - 8, TOP + PR):
            mc[m, pl.ds(r, 8), :] = zero8
    lane8 = lanes_of(8)

    def coarse(p):
        return (ca.at[p], kc.at[p - 3] if 3 <= p < 6 else None, mc)[0 if p < 3 else 1 if p < 6 else 2]

    for p in range(7):
        ref = coarse(p)
        for j in range(16):
            rows = pl.ds(TOP + 8 * j, 8)
            for m in range(2):
                ref[m, rows, :] = recv_ref[j, pl.ds((2 * p + m) * 8, 8), :]
            ref[2, rows, :] = beside(recv_ref[j, pl.ds(112, 8), :], p)
        row, count = edge_rows(p)
        for m in range(2):
            ref[m, pl.ds(TOP - count, count), :] = above_ref[pl.ds(m * TILE_ROWS + row, count), :]
            ref[m, pl.ds(TOP + PR, count), :] = below_ref[pl.ds(m * TILE_ROWS + row, count), :]
        ref[2, pl.ds(TOP - count, count), :] = beside(above_ref[pl.ds(SIDE + 3 - count, count), :], p)
        ref[2, pl.ds(TOP + PR, count), :] = beside(below_ref[pl.ds(SIDE, count), :], p)
    both = left_ref[...] + right_ref[...]
    for t in range(12):
        fa[t, 2, own, :] = start_side(both, t)
        kf[t, 2, own, :] = other_side(both, 48 + 2 * t)
    for t in range(4):
        mf[t, 2, own, :] = other_side(both, 72 + 2 * t)
    for m in range(2):
        at = m * TILE_ROWS
        for t in range(12):
            fa[t, m, pl.ds(TOP - 2, 2), :] = above_ref[pl.ds(at + 2 * t, 2), :]
            fa[t, m, pl.ds(TOP + PR, 2), :] = below_ref[pl.ds(at + 2 * t, 2), :]
            kf[t, m, pl.ds(TOP - 1, 1), :] = above_ref[pl.ds(at + 24 + t, 1), :]
            kf[t, m, pl.ds(TOP + PR, 1), :] = below_ref[pl.ds(at + 24 + t, 1), :]
        for t in range(4):
            mf[t, m, pl.ds(TOP - 1, 1), :] = above_ref[pl.ds(at + 36 + t, 1), :]
            mf[t, m, pl.ds(TOP + PR, 1), :] = below_ref[pl.ds(at + 36 + t, 1), :]
    for edge_ref, two, one, near in ((above_ref, TOP - 2, TOP - 1, 1), (below_ref, TOP + PR, TOP + PR, 0)):
        pair, single = edge_ref[pl.ds(PAIR, 2), :], edge_ref[pl.ds(PAIR + near, 1), :]
        for t in range(12):
            fa[t, 2, pl.ds(two, 2), :] = start_side(pair, t)
            kf[t, 2, pl.ds(one, 1), :] = other_side(single, 48 + 2 * t)
        for t in range(4):
            mf[t, 2, pl.ds(one, 1), :] = other_side(single, 72 + 2 * t)
    copies[0].wait()

    at_start, at_end = lane8 == 0, lane8 == 127

    def before(x):
        turned = [turn(v, 1) for v in x]
        return [jnp.where(at_start, turned[m - 1], turned[m]) for m in range(len(x))]

    def after(x):
        turned = [turn(v, 127) for v in x]
        return [jnp.where(at_end, turned[(m + 1) % 3], turned[m]) for m in range(3)]

    def mix(x, k, r, c):
        west, east = before(c), after(c)
        for m in range(3):
            part = 0.375 * c[m]
            x[0, k, m, r, :] = part + 0.125 * west[m]
            x[1, k, m, r, :] = part + 0.125 * east[m]
            x[2, k, m, r, :] = west[m] + east[m]

    def ready(i, carry):
        r = pl.ds(pl.multiple_of(8 + 8 * i, 8), 8)
        for m in range(3):
            mu = mc[m, r, :]
            mc[m, r, :] = mu + 4.0
            rc[m, r, :] = jnp.where(mu > 0.0, 1.0 / (mu + 4.0), 0.0)
            for t in range(4):
                mu = mf[t, m, r, :]
                mf[t, m, r, :] = mu + 4.0
                rf[t, m, r, :] = jnp.where(mu > 0.0, 1.0 / (mu + 4.0), 0.0)
        for k in range(3):
            mix(xa, k, r, [ca[k, m, r, :] for m in range(3)])
        return carry

    lax.fori_loop(0, PR // 8 + 2, ready, 0, unroll=18)
    for copy in copies[1:3]:
        copy.wait()

    def step(r, c_old, x_old, f_old, store_c, store_f, tiles, sums):
        here, up, down = pl.ds(r, 8), pl.ds(r - 1, 8), pl.ds(r + 1, 8)
        totals = [zero8] * 4
        for k in range(3):
            f = [[[f_old[4 * k + 2 * p + q, m, here, :] for m in range(3)] for q in range(2)] for p in range(2)]
            far = [[(before, after)[q](f[p][1 - q]) for q in range(2)] for p in range(2)]
            new = []
            for m in range(tiles):
                for q in range(2):
                    mid = 3.0 * x_old[q, k, m, here, :]
                    for p in range(2):
                        t, side = 4 * k + 2 * p + q, (up, down)[p]
                        other = f_old[4 * k + 2 * (1 - p) + q, m, side, :]
                        near = (f[1 - p][q][m] + other) + (f[p][1 - q][m] + far[p][q][m])
                        s = (kf[t, m, here, :] + near) + (mid + x_old[q, k, m, side, :])
                        store_f(t, m, s * rf[2 * p + q, m, here, :])
                        if sums and m < 2:
                            res = s - mf[2 * p + q, m, here, :] * f[p][q][m]
                            totals[2 * p + q] = totals[2 * p + q] + res * res
                c = c_old[k, m, here, :]
                near = (c_old[k, m, up, :] + c_old[k, m, down, :]) + x_old[2, k, m, here, :]
                four = (f[0][0][m] + f[0][1][m]) + (f[1][0][m] + f[1][1][m])
                s = (kc[k, m, here, :] + 0.5 * four) + near
                new.append(s * rc[m, here, :])
                if sums and m < 2:
                    res = s - mc[m, here, :] * c
                    totals[k] = totals[k] + res * res
            store_c(k, new)
        return (totals[0] + totals[1]) + (totals[2] + totals[3])

    def sweep(c_old, x_old, f_old, c_new, x_new, f_new, pending):
        def stores(r):
            rows = pl.ds(r, 8)

            def store_c(k, new):
                for m in range(3):
                    c_new[k, m, rows, :] = new[m]
                mix(x_new, k, rows, new)

            def store_f(t, m, v):
                f_new[t, m, rows, :] = v

            return store_c, store_f

        def body(i, total):
            r = pl.multiple_of(TOP + 8 * i, 8)
            return total + step(r, c_old, x_old, f_old, *stores(r), 3, True)

        half = SPLIT // 8
        total = lax.fori_loop(0, half, body, zero8, unroll=half)
        for copy in pending:
            copy.wait()
        total = lax.fori_loop(half, PR // 8, body, total, unroll=half)

        def edge(i, carry):
            r = pl.multiple_of(TOP - 8 + i * (PR + 8), 8)
            step(r, c_old, x_old, f_old, *stores(r), 3, False)
            return carry

        lax.fori_loop(0, 2, edge, 0, unroll=True)
        return total

    totals = [sweep(ca, xa, fa, cb, xb, fb, copies[3:]), sweep(cb, xb, fb, ca, xa, fa, [])]

    def last(i, total):
        r = pl.multiple_of(TOP + 8 * i, 8)

        def store_c(k, new):
            for m in range(2):
                chunk_ref[i, pl.ds((2 * k + m) * 8, 8), :] = new[m]

        def store_f(t, m, v):
            fine_ref[t, m, pl.ds(pl.multiple_of(8 * i, 8), 8), :] = v

        return total + step(r, ca, xa, fa, store_c, store_f, 2, True)

    totals.append(lax.fori_loop(0, PR // 8, last, zero8, unroll=16))
    sums = 0.0625 * jnp.concatenate([jnp.sum(v, axis=0, keepdims=True) for v in totals] + [jnp.zeros((5, 128), F32)], axis=0)
    for j in range(16):
        chunk_ref[j, pl.ds(48, 8), :] = sums


def join_kernel(fine_ref, out_hbm, block, sems):
    table = parity_table(False)
    copies = []
    for k in range(3):
        for m in range(2):
            for p in range(2):
                x = jnp.concatenate([fine_ref[4 * k + 2 * p + q, m, :, :] for q in range(2)], axis=1)
                y = permuted(x, table)
                for c in range(2):
                    block[k, 2 * m + c, pl.ds(p, PR, stride=2), :] = y[:, 128 * c : 128 * c + 128]
            for c in range(2 * m, 2 * m + 2):
                copy = pltpu.make_async_copy(
                    block.at[k, c], out_hbm.at[k, :, pl.ds(128 * c, 128)], sems.at[4 * k + c]
                )
                copy.start()
                copies.append(copy)
    for copy in copies:
        copy.wait()


def sum_kernel(recv_ref, out_ref):
    total = recv_ref[0]
    for j in range(1, 16):
        total = total + recv_ref[j]
    for i in range(8):
        out_ref[i] = total


def coarse_kernel(recv_ref, out_ref):
    for j in range(16):
        for k in range(3):
            for m in range(2):
                out_ref[k, :, pl.ds(256 * j + 128 * m, 128)] = recv_ref[j, pl.ds((2 * k + m) * 8, 8), :]


def on_device(fine_start, fine_known, fine_mu, coarse_start, coarse_known, coarse_mu):
    count_x, count_y = lax.axis_size(GX), lax.axis_size(GY)
    cell_total = 3.0 * (fine_mu.size + coarse_mu.size) * (count_x * count_y)
    chunk = pl.pallas_call(
        pack_kernel,
        out_shape=pltpu.HBM((16, MAIN, 128), F32),
        in_specs=[HBM] * 3,
        out_specs=HBM,
        scratch_shapes=[
            pltpu.VMEM(coarse_start.shape, F32),
            pltpu.VMEM(coarse_known.shape, F32),
            pltpu.VMEM(coarse_mu.shape, F32),
            pltpu.VMEM((16, MAIN, 128), F32),
            pltpu.SemaphoreType.DMA((12,)),
            pltpu.SemaphoreType.DMA((4,)),
        ],
        compiler_params=params(GRANT_KIB),
        cost_estimate=cost(2, 2e6),
        name="pack",
    )(*in_hbm(coarse_start, coarse_known, coarse_mu))
    recv = lax.all_to_all(chunk, GY, 0, 0, tiled=True)

    fs, fk, fm, low, high, top, bottom = pl.pallas_call(
        fine_kernel,
        out_shape=(
            *(pltpu.HBM((n, 2, PR, 128), F32) for n in (12, 12, 4)),
            *(pltpu.VMEM(shape, F32) for shape in ((PR, 128), (PR, 128), (2, 40, 128), (2, 40, 128))),
        ),
        in_specs=[HBM] * 3,
        out_specs=(HBM,) * 3 + (VMEM,) * 4,
        scratch_shapes=[
            pltpu.VMEM((7, 4, 2 * PR, 128), F32),
            pltpu.VMEM((28, 2, PR, 128), F32),
            pltpu.SemaphoreType.DMA((28,)),
            pltpu.SemaphoreType.DMA((7,)),
        ],
        compiler_params=params(GRANT_KIB),
        cost_estimate=cost(4, 7e6),
        name="fine",
    )(*in_hbm(fine_start, fine_known, fine_mu))

    def ahead(n):
        return [(i, i + 1) for i in range(n - 1)]

    def back(n):
        return [(i + 1, i) for i in range(n - 1)]

    left = lax.ppermute(high, GY, ahead(count_y))
    right = lax.ppermute(low, GY, back(count_y))
    up, down = pl.pallas_call(
        rows_kernel,
        grid=(1,),
        out_shape=(shaped(EDGE, 128),) * 2,
        in_specs=[pl.BlockSpec((PR, 128), lambda i: (0, 0))] * 2
        + [pl.BlockSpec((2, 40, 128), lambda i: (0, 0, 0))] * 2
        + [pl.BlockSpec((1, MAIN, 128), lambda i: (0, 0, 0)), pl.BlockSpec((1, MAIN, 128), lambda i: (15, 0, 0))],
        out_specs=(pl.BlockSpec((EDGE, 128), lambda i: (0, 0)),) * 2,
        compiler_params=params(GRANT_KIB),
        cost_estimate=cost(1, 0.3e6),
        name="rows",
    )(left, right, top, bottom, recv, recv)
    above = lax.ppermute(down, GX, ahead(count_x))
    below = lax.ppermute(up, GX, back(count_x))

    chunk, fine = pl.pallas_call(
        sweep_kernel,
        out_shape=(pltpu.VMEM((16, 56, 128), F32), pltpu.VMEM((12, 2, PR, 128), F32)),
        in_specs=[HBM] * 3 + [VMEM] * 5,
        out_specs=(VMEM, VMEM),
        scratch_shapes=[
            pltpu.VMEM((3, 3, ROWS, 128), F32),
            pltpu.VMEM((3, 3, ROWS, 128), F32),
            pltpu.VMEM((3, 3, 3, ROWS, 128), F32),
            pltpu.VMEM((3, 3, 3, ROWS, 128), F32),
            pltpu.VMEM((3, 3, ROWS, 128), F32),
            pltpu.VMEM((3, ROWS, 128), F32),
            pltpu.VMEM((3, ROWS, 128), F32),
            pltpu.VMEM((12, 3, ROWS, 128), F32),
            pltpu.VMEM((12, 3, ROWS, 128), F32),
            pltpu.VMEM((12, 3, ROWS, 128), F32),
            pltpu.VMEM((4, 3, ROWS, 128), F32),
            pltpu.VMEM((4, 3, ROWS, 128), F32),
            pltpu.SemaphoreType.DMA((5,)),
        ],
        compiler_params=params(GRANT_KIB),
        cost_estimate=cost(8, 7e6),
        name="sweeps",
    )(*in_hbm(fs, fk, fm), recv, left, right, above, below)
    out = lax.all_to_all(chunk, GY, 0, 0, tiled=True)

    fine_ghost = pl.pallas_call(
        join_kernel,
        out_shape=shaped(*fine_start.shape),
        in_specs=[VMEM],
        out_specs=HBM,
        scratch_shapes=[
            pltpu.VMEM((3, 4, 2 * PR, 128), F32),
            pltpu.SemaphoreType.DMA((12,)),
        ],
        compiler_params=params(GRANT_KIB),
        cost_estimate=cost(2, 3e6),
        name="join",
    )(fine)
    sums = pl.pallas_call(
        sum_kernel,
        grid=(1,),
        out_shape=pltpu.VMEM((8, 8, 128), F32),
        in_specs=[pl.BlockSpec((16, 8, 128), lambda i: (0, 6, 0))],
        out_specs=pl.BlockSpec((8, 8, 128), lambda i: (0, 0, 0)),
        compiler_params=params(GRANT_KIB),
        cost_estimate=cost(1, 0.1e6),
        name="sums",
    )(out)
    sums = lax.all_to_all(sums, GX, 0, 0, tiled=True)
    coarse_ghost = pl.pallas_call(
        coarse_kernel,
        out_shape=shaped(*coarse_start.shape),
        in_specs=[VMEM],
        out_specs=VMEM,
        compiler_params=params(GRANT_KIB),
        cost_estimate=cost(1, 0.8e6),
        name="coarse",
    )(out)
    norms = jnp.sqrt(jnp.sum(sums[:, :ITERS, :], axis=(0, 2)) / cell_total)
    return fine_ghost, coarse_ghost, norms


def solution(mesh):
    fine, coarse = P(None, GX, GY), P(None, BOTH, None)
    return jax.shard_map(
        on_device,
        mesh=mesh,
        in_specs=(fine, fine, P(GX, GY), coarse, coarse, P(BOTH, None)),
        out_specs=(fine, coarse, P()),
        check_vma=False,
    )
```
